256 devices in a mesh: gx: 8 (over z), gy: 4 (over x_hi, core), gz: 8 (over x_lo, y).
Axes of the slice: x: 4 (x_hi: 2, x_lo: 2; x = x_hi * 2 + x_lo), y: 4, z: 8, core: 2. Of those that a mesh axis runs over, the one named last changes fastest.
Arguments:
- density: float32 [3, 128, 256, 1024], P(None, 'gx', 'gy', 'gz'), may hold values from -6 to 6
- efficiency: float32 [128, 256, 1024], P('gx', 'gy', 'gz'), may hold values from 0.5 to 2
Outputs:
- ionized: float32 [3, 128, 256, 1024], P(None, 'gx', 'gy', 'gz')
The draws below stay inside these ranges and needn't reach their ends.
All inputs are finite; a program needn't handle non-finite values.
Results may differ from the reference program's by a relative error of at most 0.00005.
Values sent between devices are 32-bit elements; how exact they have to be, the bound alone decides.
No kernel may reach another device: no remote copies, remote signals or barrier semaphores. Data moves between devices by JAX's collectives and lax.ppermute only.
A program may use at most 128 MiB of HBM per device.

```python
import math
import jax
import jax.numpy as jnp

SNAPS = 3
R_SMALL = 4
R_LARGE = 8
NX = 128
NY = 256
NZ = 1024


def levels(key, shape, cuts, smallest, top_value):
    gain = 1.0
    for axis_at, blocks in cuts:
        steps = jax.random.uniform(jax.random.fold_in(jax.random.fold_in(key, 6), axis_at), (blocks,), jnp.float32, smallest / len(cuts), top_value / len(cuts))
        gain = gain * jnp.repeat(jnp.exp(steps), shape[axis_at] // blocks).reshape((-1,) + (1,) * (len(shape) - 1 - axis_at))
    return gain


def gaussian(own_key, dims, width, bound, split=(), kind=jnp.bfloat16):
    factor_of = levels(own_key, dims, split, -0.22, 0.18) if split else 1.0
    values = jax.random.normal(own_key, dims, jnp.float32) * width * factor_of
    return jnp.minimum(jnp.maximum(values, -bound), bound).astype(kind)


def setup_inputs(seed: int = 0) -> dict:
    splits = jax.random.split(jax.random.key(seed), 3)
    return {
        "density": gaussian(splits[0], (SNAPS, NX, NY, NZ), 1.0, 6.0, ((1, 8), (2, 4), (3, 8)), jnp.float32),
        "efficiency": jnp.clip(jnp.exp(math.log(2.0) - 1.3862944 * jax.random.uniform(splits[1], (NX, NY, NZ), jnp.float32) ** levels(splits[1], (NX, NY, NZ), ((0, 8), (1, 4), (2, 8)), -0.2, 0.2)), 0.5, 2.0),
    }


def profile(radius):
    offsets = jnp.arange(-radius, radius + 1).astype(jnp.float32)
    raw_weights = 1.0 - (offsets / (radius + 1.0)) ** 2
    return raw_weights / jnp.sqrt(jnp.sum(raw_weights * raw_weights))

def smooth(volume, radius):
    weights = profile(radius)
    for axis_dim in (3, 2, 1):
        total = jnp.zeros_like(volume)
        for index in range(2 * radius + 1):
            total = total + weights[index] * jnp.roll(volume, radius - index, axis_dim)
        volume = total
    return volume

def reference(density, efficiency):
    smooth_small = smooth(density, R_SMALL)
    smooth_large = smooth(density, R_LARGE)
    level_small = efficiency[None] * smooth_small - 0.3
    level_large = efficiency[None] * smooth_large - 0.1
    return jnp.clip(0.5 + 0.25 * jnp.maximum(level_small, level_large), 0.0, 1.0)
```

```python
import math

import jax
import jax.numpy as jnp
from jax import lax
from jax.experimental import pallas as pl
from jax.experimental.pallas import tpu as pltpu
from jax.sharding import PartitionSpec as P


R_SMALL = 4
R_LARGE = 8
H = R_LARGE
CHUNKS = ((0, 2), (2, 3))
VMEM = pl.BlockSpec(memory_space=pltpu.VMEM)
F32 = jnp.float32
BF16 = jnp.bfloat16
PARAMS = pltpu.CompilerParams(vmem_limit_bytes=24 * 2**20)


def weight(radius, k):
    return float((radius + 1) ** 2 - k * k)


def scale_of(radius):
    n = float((radius + 1) ** 2)
    total = sum((1.0 - k * k / n) ** 2 for k in range(-radius, radius + 1))
    return (1.0 / (n * math.sqrt(total))) ** 3


def near(x):
    return pltpu.with_memory_space_constraint(x, pltpu.VMEM)


def run(body, args, outs, scratch=()):
    return pl.pallas_call(
        body,
        out_shape=[pltpu.VMEM(s, F32) for s in outs],
        in_specs=[VMEM] * len(args),
        out_specs=[VMEM] * len(outs),
        scratch_shapes=list(scratch),
        compiler_params=PARAMS,
    )(*[near(a) for a in args])


def band(edge):
    shape = (256, 256)
    row = lax.broadcasted_iota(jnp.int32, shape, 0) % 128
    col = lax.broadcasted_iota(jnp.int32, shape, 1)
    z = col % 128
    if edge:
        at = jnp.where(row < 64, row - H, 128 + row - 64)
        used = row % 64 < H
        d = at - z
    else:
        d = row - z
    reach = jnp.where(col < 128, R_SMALL + 1, R_LARGE + 1)
    value = reach * reach - d * d
    keep = value > 0
    if edge:
        keep = keep & used
    return jnp.where(keep, value, 0).astype(F32).astype(BF16)


def mul(m, w):
    hi = m.astype(BF16)
    lo = (m - hi.astype(F32)).astype(BF16)
    return jnp.dot(jnp.concatenate([hi, lo], axis=1), w, preferred_element_type=F32)


def lanes(shape):
    return lax.broadcasted_iota(jnp.int32, shape, len(shape) - 1)


def edge_of(pack, p):
    return pltpu.roll(pack, (128 - H * p) % 128, 1) if p else pack


def taps(get, radius):
    total = weight(radius, 0) * get(0)
    for k in range(1, radius + 1):
        total = total + weight(radius, k) * (get(k) + get(-k))
    return total


def x_halo(total, before, after, i, n, radius):
    for a in range(radius):
        d = i + radius - a
        if d <= radius:
            total = total + weight(radius, d) * before[a]
    for b in range(radius):
        d = n + b - i
        if d <= radius:
            total = total + weight(radius, d) * after[b]
    return total


def pack_body(d, zr, zl, xeu, xed):
    s = pl.program_id(0)
    _, nx, ny, nz = d.shape
    xeu[s, :, 0:H] = d[0, nx - H :, 0:H]
    xeu[s, :, H:] = d[0, nx - H :, ny - H :]
    xed[s, :, 0:H] = d[0, 0:H, 0:H]
    xed[s, :, H:] = d[0, 0:H, ny - H :]
    lane = lanes((ny, nz))
    right = jnp.zeros((ny, nz), F32)
    left = jnp.zeros((ny, nz), F32)
    for x in range(nx):
        r = pltpu.roll(d[0, x], (H * x + H) % nz, 1)
        right = jnp.where((lane >= H * x) & (lane < H * x + H), r, right)
        at = (H * x + H) % nz
        left = jnp.where((lane >= at) & (lane < at + H), r, left)
    zr[s] = right
    zl[s] = pltpu.roll(left, nz - H, 1)


def second_body(za, zb, xzu, xzd):
    snaps, ny, nz = za.shape
    half = nz // 2
    lane = lanes((ny, nz))
    for s in range(snaps):
        xzu[s] = jnp.where(lane < half, pltpu.roll(za[s], half, 1), zb[s])
        xzd[s] = jnp.where(lane < half, za[s], pltpu.roll(zb[s], half, 1))


def slab_body(d, *outs):
    nx, ny = d.shape[1:3]
    for (low, high), up, down in zip(CHUNKS, outs[0::2], outs[1::2]):
        up[...] = d[low:high, nx - H :, H : ny - H]
        down[...] = d[low:high, 0:H, H : ny - H]


def rim_body(d, xea, xeb, xza, xzd, xzu, xzb, ws, wl, yu, yd, zs, zl):
    snaps, nx, ny, nz = d.shape
    wm, we = band(False), band(True)

    def ends(v):
        return jnp.concatenate([v[0:H], v[ny - H :]], axis=0)

    def snap(s, carry):
        packs = [ends(p[s]) for p in (xza, xzd, xzu, xzb)]
        main = [xea[s, p] for p in range(H)]
        main += [ends(d[s, x]) for x in range(nx)]
        main += [xeb[s, p] for p in range(H)]
        side = [edge_of(packs[p // H], p % H) for p in range(nx + 2 * H)]
        out = mul(jnp.concatenate(main, axis=0), wm) + mul(jnp.concatenate(side, axis=0), we)
        out = out.reshape(nx + 2 * H, 2 * H, 2 * nz)
        zs[...] = out[:, :, :nz]
        zl[...] = out[:, :, nz:]
        small = taps(lambda k: zs[H + k : H + k + nx], R_SMALL)
        large = taps(lambda k: zl[H + k : H + k + nx], R_LARGE)
        ws[s] = small
        wl[s] = large
        yu[s, 0:nx] = large[:, H:]
        yd[s, 0:nx] = large[:, 0:H]
        half = nx // 2
        yu[s, nx:, 0:R_SMALL] = small[0:half, 2 * H - R_SMALL :]
        yu[s, nx:, R_SMALL:] = small[half:, 2 * H - R_SMALL :]
        yd[s, nx:, 0:R_SMALL] = small[0:half, 0:R_SMALL]
        yd[s, nx:, R_SMALL:] = small[half:, 0:R_SMALL]
        return carry

    lax.fori_loop(0, snaps, snap, 0)


def middle_body(d, xza, xzd, xzu, xzb, acc_s, acc_l, zs, zl):
    snaps, nx, ny, nz = d.shape
    wm, we = band(False), band(True)
    inner = ny - 2 * H

    def snap(s, carry):
        for q, pack in enumerate((xza, xzd, xzu, xzb)):
            rows = pack[s, H : ny - H]
            for p in range(H):
                z = mul(edge_of(rows, p), we)
                at = q * H + p
                if H <= at < H + nx:
                    z = z + mul(d[s, at - H, H : ny - H], wm)
                zs[at] = z[:, :nz]
                zl[at] = z[:, nz:]
        for r in range(0, inner, 8):
            acc_s[s, :, r : r + 8] = taps(lambda k: zs[H + k : H + k + nx, r : r + 8], R_SMALL)
            acc_l[s, :, r : r + 8] = taps(lambda k: zl[H + k : H + k + nx, r : r + 8], R_LARGE)
        return carry

    lax.fori_loop(0, snaps, snap, 0)


def last_body(low, xia, xib, acc_s, acc_l, ws, wl, ya, yb, eff, *rest):
    out, us, ul = rest[-3:]
    j = pl.program_id(0)
    s = j + low
    nx, inner, nz = acc_s.shape[1:]
    ny = inner + 2 * H
    wm = band(False)
    scale_s, scale_l = scale_of(R_SMALL), scale_of(R_LARGE)
    half = nx // 2
    ul[:, 0:H] = ya[s, 0:nx]
    ul[:, H : 2 * H] = wl[s, :, 0:H]
    ul[:, ny : ny + H] = wl[s, :, H:]
    ul[:, ny + H :] = yb[s, 0:nx]
    us[0:half, H - R_SMALL : H] = ya[s, nx:, 0:R_SMALL]
    us[half:, H - R_SMALL : H] = ya[s, nx:, R_SMALL:]
    us[:, H : 2 * H] = ws[s, :, 0:H]
    us[:, ny : ny + H] = ws[s, :, H:]
    us[0:half, ny + H : ny + H + R_SMALL] = yb[s, nx:, 0:R_SMALL]
    us[half:, ny + H : ny + H + R_SMALL] = yb[s, nx:, R_SMALL:]
    za = mul(xia[j].reshape(H * inner, nz), wm).reshape(H, inner, 2 * nz)
    zb = mul(xib[j].reshape(H * inner, nz), wm).reshape(H, inner, 2 * nz)
    cut = H - R_SMALL
    for r in range(0, inner, 8):
        a, b = za[:, r : r + 8], zb[:, r : r + 8]
        for i in range(nx):
            us[i, 2 * H + r : 2 * H + r + 8] = x_halo(
                acc_s[s, i, r : r + 8], a[cut:, :, :nz], b[:, :, :nz], i, nx, R_SMALL
            )
            ul[i, 2 * H + r : 2 * H + r + 8] = x_halo(
                acc_l[s, i, r : r + 8], a[:, :, nz:], b[:, :, nz:], i, nx, R_LARGE
            )
    for r in range(0, ny, 8):
        small = taps(lambda k: us[:, r + H + k : r + H + k + 8], R_SMALL)
        large = taps(lambda k: ul[:, r + H + k : r + H + k + 8], R_LARGE)
        e = eff[:, r : r + 8]
        level_small = e * (small * scale_s) - 0.3
        level_large = e * (large * scale_l) - 0.1
        top = 0.5 + 0.25 * jnp.maximum(level_small, level_large)
        out[0, :, r : r + 8] = jnp.minimum(jnp.maximum(top, 0.0), 1.0)


def last(low, high, args, before, shape):
    nx, ny, nz = shape[1:]
    extra = [] if before is None else [before]
    return pl.pallas_call(
        lambda *refs: last_body(low, *refs),
        out_shape=jax.ShapeDtypeStruct(shape, F32),
        grid=(high - low,),
        in_specs=[VMEM] * len(args) + [pl.BlockSpec(memory_space=pl.ANY)] * len(extra),
        out_specs=pl.BlockSpec((1, nx, ny, nz), lambda j: (j + low, 0, 0, 0)),
        scratch_shapes=[pltpu.VMEM((nx, ny + 2 * H, nz), F32)] * 2,
        input_output_aliases={len(args): 0} if extra else {},
        compiler_params=PARAMS,
        name="last",
    )(*[near(a) for a in args], *extra)


def shift(block, axis, step):
    n = lax.axis_size(axis)
    return lax.ppermute(block, axis, [(i, (i + step) % n) for i in range(n)])


def both(axis, up, down):
    return shift(up, axis, 1), shift(down, axis, -1)


def steps(density, efficiency):
    block = density.shape
    snaps, nx, ny, nz = block
    inner = ny - 2 * H
    zpack = (snaps, ny, nz)
    xe = (snaps, H, 2 * H, nz)
    zr, zl, xeu, xed = pl.pallas_call(
        pack_body,
        out_shape=[pltpu.VMEM(s, F32) for s in (zpack, zpack, xe, xe)],
        grid=(snaps,),
        in_specs=[pl.BlockSpec((1, nx, ny, nz), lambda s: (s, 0, 0, 0))],
        out_specs=[VMEM] * 4,
        compiler_params=PARAMS,
        name="pack",
    )(density)
    za, zb = both("gz", zr, zl)
    xea, xeb = both("gx", xeu, xed)
    slabs = []
    for low, high in CHUNKS:
        slabs += [(high - low, H, inner, nz)] * 2
    slabs = run(slab_body, (density,), slabs)
    xzu, xzd = run(second_body, (za, zb), (zpack, zpack))
    xza, xzb = both("gx", xzu, xzd)
    halos = [both("gx", *slabs[2 * c : 2 * c + 2]) for c in range(len(CHUNKS))]
    wide = nx + 2 * H
    rim = [(snaps, nx, 2 * H, nz)] * 2 + [(snaps, nx + nx // 2, H, nz)] * 2
    ws, wl, yu, yd = run(
        rim_body,
        (density, xea, xeb, xza, xzd, xzu, xzb),
        rim,
        [pltpu.VMEM((wide, 2 * H, nz), F32)] * 2,
    )
    ya, yb = both("gy", yu, yd)
    acc_s, acc_l = run(
        middle_body,
        (density, xza, xzd, xzu, xzb),
        [(snaps, nx, inner, nz)] * 2,
        [pltpu.VMEM((wide, inner, nz), F32)] * 2,
    )
    out = None
    for (low, high), (xia, xib) in zip(CHUNKS, halos):
        args = (xia, xib, acc_s, acc_l, ws, wl, ya, yb, efficiency)
        out = last(low, high, args, out, block)
    return out


def solution(mesh):
    placed = (P(None, "gx", "gy", "gz"), P("gx", "gy", "gz"))
    return jax.shard_map(
        steps, mesh=mesh, in_specs=placed, out_specs=P(None, "gx", "gy", "gz"), check_vma=False
    )
```

```python
import math

import jax
import jax.numpy as jnp
from jax import lax
from jax.experimental import pallas as pl
from jax.experimental.pallas import tpu as pltpu
from jax.sharding import PartitionSpec as P


R_SMALL = 4
R_LARGE = 8
H = R_LARGE
CHUNKS = ((0, 2), (2, 3))
VMEM = pl.BlockSpec(memory_space=pltpu.VMEM)
F32 = jnp.float32
BF16 = jnp.bfloat16
PARAMS = pltpu.CompilerParams(vmem_limit_bytes=24 * 2**20)


def weight(radius, k):
    return float((radius + 1) ** 2 - k * k)


def scale_of(radius):
    n = float((radius + 1) ** 2)
    total = sum((1.0 - k * k / n) ** 2 for k in range(-radius, radius + 1))
    return (1.0 / (n * math.sqrt(total))) ** 3


def near(x):
    return pltpu.with_memory_space_constraint(x, pltpu.VMEM)


def run(body, args, outs, scratch=()):
    return pl.pallas_call(
        body,
        out_shape=[pltpu.VMEM(s, F32) for s in outs],
        in_specs=[VMEM] * len(args),
        out_specs=[VMEM] * len(outs),
        scratch_shapes=list(scratch),
        compiler_params=PARAMS,
    )(*[near(a) for a in args])


def band(edge):
    shape = (256, 256)
    row = lax.broadcasted_iota(jnp.int32, shape, 0) % 128
    col = lax.broadcasted_iota(jnp.int32, shape, 1)
    z = col % 128
    if edge:
        at = jnp.where(row < 64, row - H, 128 + row - 64)
        used = row % 64 < H
        d = at - z
    else:
        d = row - z
    reach = jnp.where(col < 128, R_SMALL + 1, R_LARGE + 1)
    value = reach * reach - d * d
    keep = value > 0
    if edge:
        keep = keep & used
    return jnp.where(keep, value, 0).astype(F32).astype(BF16)


def mul(m, w):
    hi = m.astype(BF16)
    lo = (m - hi.astype(F32)).astype(BF16)
    return jnp.dot(jnp.concatenate([hi, lo], axis=1), w, preferred_element_type=F32)


def lanes(shape):
    return lax.broadcasted_iota(jnp.int32, shape, len(shape) - 1)


def edge_of(pack, p):
    return pltpu.roll(pack, (128 - H * p) % 128, 1) if p else pack


def taps(get, radius):
    total = weight(radius, 0) * get(0)
    for k in range(1, radius + 1):
        total = total + weight(radius, k) * (get(k) + get(-k))
    return total


def rows_band(radius, ny):
    wide = ny + 2 * H
    y = lax.broadcasted_iota(jnp.int32, (ny, 2 * wide), 0)
    c = lax.broadcasted_iota(jnp.int32, (ny, 2 * wide), 1)
    d = jnp.where(c < wide, c, c - wide) - H - y
    value = (radius + 1) ** 2 - d * d
    return jnp.where(value > 0, value, 0).astype(F32).astype(BF16)


def stack(m):
    hi = m.astype(BF16)
    lo = (m - hi.astype(F32)).astype(BF16)
    return jnp.concatenate([hi, lo], axis=0)


def x_halo(total, before, after, i, n, radius):
    for a in range(radius):
        d = i + radius - a
        if d <= radius:
            total = total + weight(radius, d) * before[a]
    for b in range(radius):
        d = n + b - i
        if d <= radius:
            total = total + weight(radius, d) * after[b]
    return total


def pack_body(d_hbm, zr, zl, xeu, xed, d_all, sems):
    snaps, nx, ny, nz = d_all.shape
    copies = [
        pltpu.make_async_copy(d_hbm.at[s], d_all.at[s], sems.at[s]) for s in range(snaps)
    ]
    for copy in copies:
        copy.start()
    lane = lanes((ny, nz))
    for s in range(snaps):
        copies[s].wait()
        d = d_all.at[s]
        xeu[s, :, 0:H] = d[nx - H :, 0:H]
        xeu[s, :, H:] = d[nx - H :, ny - H :]
        xed[s, :, 0:H] = d[0:H, 0:H]
        xed[s, :, H:] = d[0:H, ny - H :]
        right = jnp.zeros((ny, nz), F32)
        left = jnp.zeros((ny, nz), F32)
        for x in range(nx):
            r = pltpu.roll(d[x], (H * x + H) % nz, 1)
            right = jnp.where((lane >= H * x) & (lane < H * x + H), r, right)
            at = (H * x + H) % nz
            left = jnp.where((lane >= at) & (lane < at + H), r, left)
        zr[s] = right
        zl[s] = pltpu.roll(left, nz - H, 1)


def second_body(za, zb, xzu, xzd):
    snaps, ny, nz = za.shape
    half = nz // 2
    lane = lanes((ny, nz))
    for s in range(snaps):
        xzu[s] = jnp.where(lane < half, pltpu.roll(za[s], half, 1), zb[s])
        xzd[s] = jnp.where(lane < half, za[s], pltpu.roll(zb[s], half, 1))


def slab_body(d, *outs):
    nx, ny = d.shape[1:3]
    for (low, high), up, down in zip(CHUNKS, outs[0::2], outs[1::2]):
        up[...] = d[low:high, nx - H :, H : ny - H]
        down[...] = d[low:high, 0:H, H : ny - H]


def put(ref, s, i, r, value):
    ref[s, i, r : r + 8] = value


def x_sums(planes, store, radius):
    n = planes.shape[0] - 2 * H
    v = [planes[j] for j in range(n + 2 * H)]
    for i in range(n):
        store(i, taps(lambda k: v[H + i + k], radius))


def rim_body(d, xea, xeb, xza, xzd, xzu, xzb, ws, wl, yu, yd):
    snaps, nx, ny, nz = d.shape
    wm, we = band(False), band(True)

    def ends(v):
        return jnp.concatenate([v[0:H], v[ny - H :]], axis=0)

    for s in range(snaps):
        packs = [ends(p[s]) for p in (xza, xzd, xzu, xzb)]
        main = [xea[s, p] for p in range(H)]
        main += [ends(d[s, x]) for x in range(nx)]
        main += [xeb[s, p] for p in range(H)]
        side = [edge_of(packs[p // H], p % H) for p in range(nx + 2 * H)]
        out = mul(jnp.concatenate(main, axis=0), wm) + mul(jnp.concatenate(side, axis=0), we)
        out = out.reshape(nx + 2 * H, 2 * H, 2 * nz)
        for r in (0, H):
            x_sums(out[:, r : r + 8, :nz], lambda i, v: put(ws, s, i, r, v), R_SMALL)
            x_sums(out[:, r : r + 8, nz:], lambda i, v: put(wl, s, i, r, v), R_LARGE)
        small, large = ws[s], wl[s]
        yu[s, 0:nx] = large[:, H:]
        yd[s, 0:nx] = large[:, 0:H]
        half = nx // 2
        yu[s, nx:, 0:R_SMALL] = small[0:half, 2 * H - R_SMALL :]
        yu[s, nx:, R_SMALL:] = small[half:, 2 * H - R_SMALL :]
        yd[s, nx:, 0:R_SMALL] = small[0:half, 0:R_SMALL]
        yd[s, nx:, R_SMALL:] = small[half:, 0:R_SMALL]


def middle_body(d, xza, xzd, xzu, xzb, acc_s, acc_l, zs_all, zl_all):
    snaps, nx, ny, nz = d.shape
    wm, we = band(False), band(True)
    inner = ny - 2 * H

    for s in range(snaps):
        zs, zl = zs_all.at[s], zl_all.at[s]
        side = [edge_of(p[s, H : ny - H], k) for p in (xza, xzd, xzu, xzb) for k in range(H)]
        edge = mul(jnp.concatenate(side, axis=0), we).reshape(nx + 2 * H, inner, 2 * nz)
        main = mul(d[s, :, H : ny - H].reshape(nx * inner, nz), wm).reshape(nx, inner, 2 * nz)
        for ref, cut in ((zs, slice(0, nz)), (zl, slice(nz, 2 * nz))):
            ref[0:H] = edge[0:H, :, cut]
            ref[H : H + nx] = edge[H : H + nx, :, cut] + main[:, :, cut]
            ref[H + nx :] = edge[H + nx :, :, cut]
        for r in range(0, inner, 8):
            x_sums(zs[:, r : r + 8], lambda i, v: put(acc_s, s, i, r, v), R_SMALL)
            x_sums(zl[:, r : r + 8], lambda i, v: put(acc_l, s, i, r, v), R_LARGE)


def fill_body(low, xia, xib, acc_s, acc_l, us, ul):
    n, _, _, _ = us.shape
    wm = band(False)
    for j in range(n):
        add_planes(xia[j], xib[j], acc_s.at[low + j], acc_l.at[low + j], us.at[j], ul.at[j], 0, wm)


def add_planes(xia, xib, acc_s, acc_l, us, ul, first, wm):
    nx, inner, nz = acc_s.shape
    cut = H - R_SMALL
    za = mul(xia.reshape(H * inner, nz), wm).reshape(H, inner, 2 * nz)
    zb = mul(xib.reshape(H * inner, nz), wm).reshape(H, inner, 2 * nz)
    for r in range(0, inner, 8):
        a, b = za[:, r : r + 8], zb[:, r : r + 8]
        at = slice(first + r, first + r + 8)
        for i in range(nx):
            us[i, at] = x_halo(
                acc_s[i, r : r + 8], a[cut:, :, :nz], b[:, :, :nz], i, nx, R_SMALL
            )
            ul[i, at] = x_halo(acc_l[i, r : r + 8], a[:, :, nz:], b[:, :, nz:], i, nx, R_LARGE)


def last_body(low, fused, *refs):
    if fused:
        xia, xib = refs[:2]
        refs = refs[2:]
    u_s, u_l, ws, wl, ya, yb, eff, *rest = refs
    out, us, ul = rest[-3:]
    j = pl.program_id(0)
    s = j + low
    nx, inner, nz = u_s.shape[1:]
    ny = inner + 2 * H
    half = nx // 2
    if fused:
        add_planes(xia[j], xib[j], u_s.at[s], u_l.at[s], us, ul, 2 * H, band(False))
    else:
        us[:, 2 * H : ny] = u_s[j]
        ul[:, 2 * H : ny] = u_l[j]
    ul[:, 0:H] = ya[s, 0:nx]
    ul[:, H : 2 * H] = wl[s, :, 0:H]
    ul[:, ny : ny + H] = wl[s, :, H:]
    ul[:, ny + H :] = yb[s, 0:nx]
    us[:, 0:H] = jnp.zeros((nx, H, nz), F32)
    us[:, ny + H :] = jnp.zeros((nx, H, nz), F32)
    us[0:half, H - R_SMALL : H] = ya[s, nx:, 0:R_SMALL]
    us[half:, H - R_SMALL : H] = ya[s, nx:, R_SMALL:]
    us[:, H : 2 * H] = ws[s, :, 0:H]
    us[:, ny : ny + H] = ws[s, :, H:]
    us[0:half, ny + H : ny + H + R_SMALL] = yb[s, nx:, 0:R_SMALL]
    us[half:, ny + H : ny + H + R_SMALL] = yb[s, nx:, R_SMALL:]
    band_s, band_l = rows_band(R_SMALL, ny), rows_band(R_LARGE, ny)
    scale_s, scale_l = 0.25 * scale_of(R_SMALL), 0.25 * scale_of(R_LARGE)

    def y_sum(ref, w, i):
        pair = jnp.concatenate([stack(ref[i]), stack(ref[i + half])], axis=1)
        return jnp.dot(w, pair, preferred_element_type=F32)

    for i in range(half):
        small, large = y_sum(us, band_s, i), y_sum(ul, band_l, i)
        for at, col in ((i, slice(0, nz)), (i + half, slice(nz, 2 * nz))):
            e = eff[at]
            low_r = e * (small[:, col] * scale_s) + (0.5 - 0.25 * 0.3)
            high_r = e * (large[:, col] * scale_l) + (0.5 - 0.25 * 0.1)
            out[0, at] = jnp.minimum(jnp.maximum(jnp.maximum(low_r, high_r), 0.0), 1.0)


def last(low, high, fused, args, before, shape):
    nx, ny, nz = shape[1:]
    extra = [] if before is None else [before]
    return pl.pallas_call(
        lambda *refs: last_body(low, fused, *refs),
        out_shape=jax.ShapeDtypeStruct(shape, F32),
        grid=(high - low,),
        in_specs=[VMEM] * len(args) + [pl.BlockSpec(memory_space=pl.ANY)] * len(extra),
        out_specs=pl.BlockSpec((1, nx, ny, nz), lambda j: (j + low, 0, 0, 0)),
        scratch_shapes=[pltpu.VMEM((nx, ny + 2 * H, nz), F32)] * 2,
        input_output_aliases={len(args): 0} if extra else {},
        compiler_params=PARAMS,
        name="last",
    )(*[near(a) for a in args], *extra)


def shift(block, axis, step):
    n = lax.axis_size(axis)
    return lax.ppermute(block, axis, [(i, (i + step) % n) for i in range(n)])


def both(axis, up, down):
    return shift(up, axis, 1), shift(down, axis, -1)


def steps(density, efficiency):
    block = density.shape
    snaps, nx, ny, nz = block
    inner = ny - 2 * H
    zpack = (snaps, ny, nz)
    xe = (snaps, H, 2 * H, nz)
    zr, zl, xeu, xed = pl.pallas_call(
        pack_body,
        out_shape=[pltpu.VMEM(s, F32) for s in (zpack, zpack, xe, xe)],
        in_specs=[pl.BlockSpec(memory_space=pl.ANY)],
        out_specs=[VMEM] * 4,
        scratch_shapes=[pltpu.VMEM(block, F32), pltpu.SemaphoreType.DMA((snaps,))],
        compiler_params=PARAMS,
        name="pack",
    )(pltpu.with_memory_space_constraint(density, pltpu.HBM))
    za, zb = both("gz", zr, zl)
    xea, xeb = both("gx", xeu, xed)
    slabs = []
    for low, high in CHUNKS:
        slabs += [(high - low, H, inner, nz)] * 2
    slabs = run(slab_body, (density,), slabs)
    xzu, xzd = run(second_body, (za, zb), (zpack, zpack))
    xza, xzb = both("gx", xzu, xzd)
    halos = [both("gx", *slabs[2 * c : 2 * c + 2]) for c in range(len(CHUNKS))]
    wide = nx + 2 * H
    rim = [(snaps, nx, 2 * H, nz)] * 2 + [(snaps, nx + nx // 2, H, nz)] * 2
    ws, wl, yu, yd = run(rim_body, (density, xea, xeb, xza, xzd, xzu, xzb), rim)
    ya, yb = both("gy", yu, yd)
    acc_s, acc_l = run(
        middle_body,
        (density, xza, xzd, xzu, xzb),
        [(snaps, nx, inner, nz)] * 2,
        [pltpu.VMEM((snaps, wide, inner, nz), F32)] * 2,
    )
    out = None
    for c, ((low, high), (xia, xib)) in enumerate(zip(CHUNKS, halos)):
        rest = (ws, wl, ya, yb, efficiency)
        if c == len(CHUNKS) - 1:
            out = last(low, high, True, (xia, xib, acc_s, acc_l) + rest, out, block)
        else:
            part = [(high - low, nx, inner, nz)] * 2
            filled = run(lambda *refs: fill_body(low, *refs), (xia, xib, acc_s, acc_l), part)
            out = last(low, high, False, tuple(filled) + rest, out, block)
    return out


def solution(mesh):
    placed = (P(None, "gx", "gy", "gz"), P("gx", "gy", "gz"))
    return jax.shard_map(
        steps, mesh=mesh, in_specs=placed, out_specs=P(None, "gx", "gy", "gz"), check_vma=False
    )
```

```python
import math

import jax
import jax.numpy as jnp
from jax import lax
from jax.experimental import pallas as pl
from jax.experimental.pallas import tpu as pltpu
from jax.sharding import PartitionSpec as P


R_SMALL = 4
R_LARGE = 8
H = R_LARGE
CHUNKS = ((0, 2), (2, 3))
VMEM = pl.BlockSpec(memory_space=pltpu.VMEM)
F32 = jnp.float32
BF16 = jnp.bfloat16
PARAMS = pltpu.CompilerParams(vmem_limit_bytes=24 * 2**20)


def weight(radius, k):
    return float((radius + 1) ** 2 - k * k)


def scale_of(radius):
    n = float((radius + 1) ** 2)
    total = sum((1.0 - k * k / n) ** 2 for k in range(-radius, radius + 1))
    return (1.0 / (n * math.sqrt(total))) ** 3


def near(x):
    return pltpu.with_memory_space_constraint(x, pltpu.VMEM)


def run(body, args, outs, scratch=()):
    return pl.pallas_call(
        body,
        out_shape=[pltpu.VMEM(s, F32) for s in outs],
        in_specs=[VMEM] * len(args),
        out_specs=[VMEM] * len(outs),
        scratch_shapes=list(scratch),
        compiler_params=PARAMS,
    )(*[near(a) for a in args])


def band(edge):
    shape = (256, 256)
    row = lax.broadcasted_iota(jnp.int32, shape, 0) % 128
    col = lax.broadcasted_iota(jnp.int32, shape, 1)
    z = col % 128
    if edge:
        at = jnp.where(row < 64, row - H, 128 + row - 64)
        used = row % 64 < H
        d = at - z
    else:
        d = row - z
    reach = jnp.where(col < 128, R_SMALL + 1, R_LARGE + 1)
    value = reach * reach - d * d
    keep = value > 0
    if edge:
        keep = keep & used
    return jnp.where(keep, value, 0).astype(F32).astype(BF16)


def mul(m, w):
    hi = m.astype(BF16)
    lo = (m - hi.astype(F32)).astype(BF16)
    return jnp.dot(jnp.concatenate([hi, lo], axis=1), w, preferred_element_type=F32)


def lanes(shape):
    return lax.broadcasted_iota(jnp.int32, shape, len(shape) - 1)


def edge_of(pack, p):
    return pltpu.roll(pack, (128 - H * p) % 128, 1) if p else pack


def taps(get, radius):
    total = weight(radius, 0) * get(0)
    for k in range(1, radius + 1):
        total = total + weight(radius, k) * (get(k) + get(-k))
    return total


def rows_band(radius, ny):
    y = lax.broadcasted_iota(jnp.int32, (ny, 2 * ny), 0)
    c = lax.broadcasted_iota(jnp.int32, (ny, 2 * ny), 1)
    d = jnp.where(c < ny, c, c - ny) - y
    value = (radius + 1) ** 2 - d * d
    return jnp.where(value > 0, value, 0).astype(F32).astype(BF16)


def ends_band():
    y = lax.broadcasted_iota(jnp.int32, (4 * H, 8 * H), 0)
    c = lax.broadcasted_iota(jnp.int32, (4 * H, 8 * H), 1)
    reach = jnp.where(y < 2 * H, R_SMALL + 1, R_LARGE + 1)
    same = (y < 2 * H) == (c < 4 * H)
    row, col = y % (2 * H), c % (2 * H)
    top = (row < H) == (col < H)
    d = jnp.where(row < H, col - H - row, col - row + H)
    value = reach * reach - d * d
    return jnp.where(same & top & (value > 0), value, 0).astype(F32).astype(BF16)


def level(small, large, e):
    low = e * (small * (0.25 * scale_of(R_SMALL))) + (0.5 - 0.25 * 0.3)
    high = e * (large * (0.25 * scale_of(R_LARGE))) + (0.5 - 0.25 * 0.1)
    return jnp.minimum(jnp.maximum(jnp.maximum(low, high), 0.0), 1.0)


def stack(m):
    hi = m.astype(BF16)
    lo = (m - hi.astype(F32)).astype(BF16)
    return jnp.concatenate([hi, lo], axis=0)


def x_halo(total, before, after, i, n, radius):
    for a in range(radius):
        d = i + radius - a
        if d <= radius:
            total = total + weight(radius, d) * before[a]
    for b in range(radius):
        d = n + b - i
        if d <= radius:
            total = total + weight(radius, d) * after[b]
    return total


def pack_body(d_hbm, d, zr, zl, xeu, xed, sems):
    snaps, nx, ny, nz = d.shape
    parts = [(s, p * H) for s in range(snaps) for p in range(nx // H)]
    copies = [
        pltpu.make_async_copy(d_hbm.at[s, pl.ds(p, H)], d.at[s, pl.ds(p, H)], sems.at[k])
        for k, (s, p) in enumerate(parts)
    ]
    for copy in copies:
        copy.start()
    lane = lanes((ny, nz))
    for (s, p), copy in zip(parts, copies):
        copy.wait()
        if p == 0:
            right = jnp.zeros((ny, nz), F32)
            left = jnp.zeros((ny, nz), F32)
            xed[s, :, 0:H] = d[s, 0:H, 0:H]
            xed[s, :, H:] = d[s, 0:H, ny - H :]
        if p == nx - H:
            xeu[s, :, 0:H] = d[s, p:, 0:H]
            xeu[s, :, H:] = d[s, p:, ny - H :]
        for x in range(p, p + H):
            r = pltpu.roll(d[s, x], (H * x + H) % nz, 1)
            right = jnp.where((lane >= H * x) & (lane < H * x + H), r, right)
            at = (H * x + H) % nz
            left = jnp.where((lane >= at) & (lane < at + H), r, left)
        if p == nx - H:
            zr[s] = right
            zl[s] = pltpu.roll(left, nz - H, 1)


def second_body(za, zb, xzu, xzd):
    snaps, ny, nz = za.shape
    half = nz // 2
    lane = lanes((ny, nz))
    for s in range(snaps):
        xzu[s] = jnp.where(lane < half, pltpu.roll(za[s], half, 1), zb[s])
        xzd[s] = jnp.where(lane < half, za[s], pltpu.roll(zb[s], half, 1))


def slab_body(d, *outs):
    nx, ny = d.shape[1:3]
    for (low, high), up, down in zip(CHUNKS, outs[0::2], outs[1::2]):
        up[...] = d[low:high, nx - H :, H : ny - H]
        down[...] = d[low:high, 0:H, H : ny - H]


def put(ref, s, i, r, value):
    ref[s, i, r : r + 8] = value


def x_sums(planes, store, radius):
    n = planes.shape[0] - 2 * H
    v = [planes[j] for j in range(n + 2 * H)]
    for i in range(n):
        store(i, taps(lambda k: v[H + i + k], radius))


def rim_body(d, xea, xeb, xza, xzd, xzu, xzb, ws, wl, yu, yd):
    snaps, nx, ny, nz = d.shape
    wm, we = band(False), band(True)

    def ends(v):
        return jnp.concatenate([v[0:H], v[ny - H :]], axis=0)

    for s in range(snaps):
        packs = [ends(p[s]) for p in (xza, xzd, xzu, xzb)]
        main = [xea[s, p] for p in range(H)]
        main += [ends(d[s, x]) for x in range(nx)]
        main += [xeb[s, p] for p in range(H)]
        side = [edge_of(packs[p // H], p % H) for p in range(nx + 2 * H)]
        out = mul(jnp.concatenate(main, axis=0), wm) + mul(jnp.concatenate(side, axis=0), we)
        out = out.reshape(nx + 2 * H, 2 * H, 2 * nz)
        for r in (0, H):
            x_sums(out[:, r : r + 8, :nz], lambda i, v: put(ws, s, i, r, v), R_SMALL)
            x_sums(out[:, r : r + 8, nz:], lambda i, v: put(wl, s, i, r, v), R_LARGE)
        small, large = ws[s], wl[s]
        yu[s, 0:nx] = large[:, H:]
        yd[s, 0:nx] = large[:, 0:H]
        half = nx // 2
        yu[s, nx:, 0:R_SMALL] = small[0:half, 2 * H - R_SMALL :]
        yu[s, nx:, R_SMALL:] = small[half:, 2 * H - R_SMALL :]
        yd[s, nx:, 0:R_SMALL] = small[0:half, 0:R_SMALL]
        yd[s, nx:, R_SMALL:] = small[half:, 0:R_SMALL]


def middle_body(d, xza, xzd, xzu, xzb, acc_s, acc_l, zs_all, zl_all):
    snaps, nx, ny, nz = d.shape
    wm, we = band(False), band(True)
    inner = ny - 2 * H

    for s in range(snaps):
        zs, zl = zs_all.at[s], zl_all.at[s]
        side = [edge_of(p[s, H : ny - H], k) for p in (xza, xzd, xzu, xzb) for k in range(H)]
        edge = mul(jnp.concatenate(side, axis=0), we).reshape(nx + 2 * H, inner, 2 * nz)
        main = mul(d[s, :, H : ny - H].reshape(nx * inner, nz), wm).reshape(nx, inner, 2 * nz)
        for ref, cut in ((zs, slice(0, nz)), (zl, slice(nz, 2 * nz))):
            ref[0:H] = edge[0:H, :, cut]
            ref[H : H + nx] = edge[H : H + nx, :, cut] + main[:, :, cut]
            ref[H + nx :] = edge[H + nx :, :, cut]
        for r in range(0, inner, 8):
            x_sums(zs[:, r : r + 8], lambda i, v: put(acc_s, s, i, r, v), R_SMALL)
            x_sums(zl[:, r : r + 8], lambda i, v: put(acc_l, s, i, r, v), R_LARGE)


def add_planes(xia, xib, acc_s, acc_l, us, ul, first, wm):
    nx, inner, nz = acc_s.shape
    cut = H - R_SMALL
    za = mul(xia.reshape(H * inner, nz), wm).reshape(H, inner, 2 * nz)
    zb = mul(xib.reshape(H * inner, nz), wm).reshape(H, inner, 2 * nz)
    for r in range(0, inner, 8):
        a, b = za[:, r : r + 8], zb[:, r : r + 8]
        at = slice(first + r, first + r + 8)
        for i in range(nx):
            us[i, at] = x_halo(
                acc_s[i, r : r + 8], a[cut:, :, :nz], b[:, :, :nz], i, nx, R_SMALL
            )
            ul[i, at] = x_halo(acc_l[i, r : r + 8], a[:, :, nz:], b[:, :, nz:], i, nx, R_LARGE)


def own_sums(us, ul, band_s, band_l, i):
    half = us.shape[0] // 2
    sums = []
    for ref, w in ((us, band_s), (ul, band_l)):
        pair = jnp.concatenate([stack(ref[i]), stack(ref[i + half])], axis=1)
        sums.append(jnp.dot(w, pair, preferred_element_type=F32))
    return sums


def halo_sums(ya, yb, s, i, half, w):
    top, bottom = ya[s, 2 * half + i], yb[s, 2 * half + i]
    first = jnp.concatenate([pltpu.roll(top, R_SMALL, 0), bottom], axis=0)
    second = jnp.concatenate([top, pltpu.roll(bottom, R_SMALL, 0)], axis=0)
    cols = []
    for at, small in ((i, first), (i + half, second)):
        large = jnp.concatenate([ya[s, at], yb[s, at]], axis=0)
        cols.append(jnp.concatenate([stack(small), stack(large)], axis=0))
    return jnp.dot(w, jnp.concatenate(cols, axis=1), preferred_element_type=F32)


def rim_rows(v):
    return jnp.concatenate([v[0:H], v[v.shape[0] - H :]], axis=0)


def prepare(xia, xib, acc_s, acc_l, ws, wl, us, ul, wm):
    ny = us.shape[1]
    add_planes(xia, xib, acc_s, acc_l, us, ul, H, wm)
    for ref, w in ((us, ws), (ul, wl)):
        ref[:, 0:H] = w[:, 0:H]
        ref[:, ny - H :] = w[:, H:]


def inner_body(low, xia, xib, acc_s, acc_l, ws, wl, eff, out, es, el, us, ul, done, sems):
    n, nx, ny, nz = us.shape
    half = nx // 2
    rows = slice(H, ny - H)
    wm = band(False)
    band_s, band_l = rows_band(R_SMALL, ny), rows_band(R_LARGE, ny)
    copies = []
    for j in range(n):
        s = low + j
        here = (acc_s.at[s], acc_l.at[s], ws.at[s], wl.at[s], us.at[j], ul.at[j])
        prepare(xia[j], xib[j], *here, wm)
        for i in range(half):
            sums = own_sums(us.at[j], ul.at[j], band_s, band_l, i)
            for at, col in ((i, slice(0, nz)), (i + half, slice(nz, 2 * nz))):
                small, large = sums[0][:, col], sums[1][:, col]
                done[j, at] = level(small[rows], large[rows], eff[at, rows])
                es[j, at] = rim_rows(small)
                el[j, at] = rim_rows(large)
        copy = pltpu.make_async_copy(done.at[j], out.at[s, :, pl.ds(H, ny - 2 * H), :], sems.at[j])
        copy.start()
        copies.append(copy)
    for copy in copies:
        copy.wait()


def final_body(low, xia, xib, acc_s, acc_l, ws, wl, eff, ya, yb, es, el, _, out, us, ul, rim, done, sems):
    n, nx, ny, nz = us.shape
    half = nx // 2
    wm, w = band(False), ends_band()
    band_s, band_l = rows_band(R_SMALL, ny), rows_band(R_LARGE, ny)
    sides = ((0, slice(0, nz)), (half, slice(nz, 2 * nz)))
    copies = []
    for j in range(n):
        s = low + j
        here = (acc_s.at[s], acc_l.at[s], ws.at[s], wl.at[s], us.at[j], ul.at[j])
        prepare(xia[j], xib[j], *here, wm)
        for i in range(half):
            sums = own_sums(us.at[j], ul.at[j], band_s, band_l, i)
            more = halo_sums(ya, yb, s, i, half, w)
            for step, col in sides:
                at = i + step
                small, large = sums[0][:, col], sums[1][:, col]
                add_s, add_l = more[0 : 2 * H, col], more[2 * H :, col]
                rows = slice(H, ny - H)
                done[j, at, rows] = level(small[rows], large[rows], eff[at, rows])
                ends = level(rim_rows(small) + add_s, rim_rows(large) + add_l, rim_rows(eff[at]))
                done[j, at, 0:H] = ends[0:H]
                done[j, at, ny - H :] = ends[H:]
        copies.append(pltpu.make_async_copy(done.at[j], out.at[s], sems.at[len(copies)]))
        copies[-1].start()
    for s in range(low):
        for i in range(half):
            more = halo_sums(ya, yb, s, i, half, w)
            for step, col in sides:
                at = i + step
                add_s, add_l = more[0 : 2 * H, col], more[2 * H :, col]
                rim[s, at] = level(es[s, at] + add_s, el[s, at] + add_l, rim_rows(eff[at]))
        for k, start in enumerate((0, ny - H)):
            source = rim.at[s, :, pl.ds(k * H, H), :]
            target = out.at[s, :, pl.ds(start, H), :]
            copies.append(pltpu.make_async_copy(source, target, sems.at[len(copies)]))
            copies[-1].start()
    for copy in copies:
        copy.wait()


def inner_call(high, args, shape):
    _, nx, ny, nz = shape
    ends = (high, nx, 2 * H, nz)
    return pl.pallas_call(
        lambda *refs: inner_body(0, *refs),
        out_shape=[jax.ShapeDtypeStruct(shape, F32), pltpu.VMEM(ends, F32), pltpu.VMEM(ends, F32)],
        in_specs=[VMEM] * len(args),
        out_specs=[pl.BlockSpec(memory_space=pl.ANY), VMEM, VMEM],
        scratch_shapes=[pltpu.VMEM((high, nx, ny, nz), F32)] * 2
        + [pltpu.VMEM((high, nx, ny - 2 * H, nz), F32), pltpu.SemaphoreType.DMA((high,))],
        compiler_params=PARAMS,
        name="inner",
    )(*[near(a) for a in args])


def final_call(low, args, before, shape):
    snaps, nx, ny, nz = shape
    n = snaps - low
    any_space = pl.BlockSpec(memory_space=pl.ANY)
    return pl.pallas_call(
        lambda *refs: final_body(low, *refs),
        out_shape=jax.ShapeDtypeStruct(shape, F32),
        in_specs=[VMEM] * len(args) + [any_space],
        out_specs=any_space,
        scratch_shapes=[pltpu.VMEM((n, nx, ny, nz), F32)] * 2
        + [pltpu.VMEM((low, nx, 2 * H, nz), F32), pltpu.VMEM((n, nx, ny, nz), F32)]
        + [pltpu.SemaphoreType.DMA((n + 2 * low,))],
        input_output_aliases={len(args): 0},
        compiler_params=PARAMS,
        name="final",
    )(*[near(a) for a in args], before)


def shift(block, axis, step):
    n = lax.axis_size(axis)
    return lax.ppermute(block, axis, [(i, (i + step) % n) for i in range(n)])


def both(axis, up, down):
    return shift(up, axis, 1), shift(down, axis, -1)


def steps(density, efficiency):
    block = density.shape
    snaps, nx, ny, nz = block
    inner = ny - 2 * H
    zpack = (snaps, ny, nz)
    xe = (snaps, H, 2 * H, nz)
    own, zr, zl, xeu, xed = pl.pallas_call(
        pack_body,
        out_shape=[pltpu.VMEM(s, F32) for s in (block, zpack, zpack, xe, xe)],
        in_specs=[pl.BlockSpec(memory_space=pl.ANY)],
        out_specs=[VMEM] * 5,
        scratch_shapes=[pltpu.SemaphoreType.DMA((snaps * nx // H,))],
        compiler_params=PARAMS,
        name="pack",
    )(pltpu.with_memory_space_constraint(density, pltpu.HBM))
    za, zb = both("gz", zr, zl)
    xea, xeb = both("gx", xeu, xed)
    slabs = []
    for low, high in CHUNKS:
        slabs += [(high - low, H, inner, nz)] * 2
    slabs = run(slab_body, (own,), slabs)
    xzu, xzd = run(second_body, (za, zb), (zpack, zpack))
    xza, xzb = both("gx", xzu, xzd)
    halos = [both("gx", *slabs[2 * c : 2 * c + 2]) for c in range(len(CHUNKS))]
    wide = nx + 2 * H
    rim = [(snaps, nx, 2 * H, nz)] * 2 + [(snaps, nx + nx // 2, H, nz)] * 2
    ws, wl, yu, yd = run(rim_body, (own, xea, xeb, xza, xzd, xzu, xzb), rim)
    ya, yb = both("gy", yu, yd)
    acc_s, acc_l = run(
        middle_body,
        (own, xza, xzd, xzu, xzb),
        [(snaps, nx, inner, nz)] * 2,
        [pltpu.VMEM((snaps, wide, inner, nz), F32)] * 2,
    )
    shared = (acc_s, acc_l, ws, wl, efficiency)
    (_, split_at), _ = CHUNKS
    out, es, el = inner_call(split_at, halos[0] + shared, block)
    out = final_call(split_at, halos[1] + shared + (ya, yb, es, el), out, block)
    return out


def solution(mesh):
    placed = (P(None, "gx", "gy", "gz"), P("gx", "gy", "gz"))
    return jax.shard_map(
        steps, mesh=mesh, in_specs=placed, out_specs=P(None, "gx", "gy", "gz"), check_vma=False
    )
```

```python
import math

import jax
import jax.numpy as jnp
from jax import lax
from jax.experimental import pallas as pl
from jax.experimental.pallas import tpu as pltpu
from jax.sharding import PartitionSpec as P


R_SMALL = 4
R_LARGE = 8
H = R_LARGE
LATE = 3
VMEM = pl.BlockSpec(memory_space=pltpu.VMEM)
F32 = jnp.float32
BF16 = jnp.bfloat16
PARAMS = pltpu.CompilerParams(vmem_limit_bytes=24 * 2**20)


def weight(radius, k):
    return float((radius + 1) ** 2 - k * k)


def scale_of(radius):
    n = float((radius + 1) ** 2)
    total = sum((1.0 - k * k / n) ** 2 for k in range(-radius, radius + 1))
    return (1.0 / (n * math.sqrt(total))) ** 3


def near(x):
    return pltpu.with_memory_space_constraint(x, pltpu.VMEM)


def run(body, args, outs, scratch=()):
    return pl.pallas_call(
        body,
        out_shape=[pltpu.VMEM(s, F32) for s in outs],
        in_specs=[VMEM] * len(args),
        out_specs=[VMEM] * len(outs),
        scratch_shapes=list(scratch),
        compiler_params=PARAMS,
    )(*[near(a) for a in args])


def band(edge):
    shape = (256, 256)
    row = lax.broadcasted_iota(jnp.int32, shape, 0) % 128
    col = lax.broadcasted_iota(jnp.int32, shape, 1)
    z = col % 128
    if edge:
        at = jnp.where(row < 64, row - H, 128 + row - 64)
        used = row % 64 < H
        d = at - z
    else:
        d = row - z
    reach = jnp.where(col < 128, R_SMALL + 1, R_LARGE + 1)
    value = reach * reach - d * d
    keep = value > 0
    if edge:
        keep = keep & used
    return jnp.where(keep, value, 0).astype(F32).astype(BF16)


def mul(m, w):
    hi = m.astype(BF16)
    lo = (m - hi.astype(F32)).astype(BF16)
    return jnp.dot(jnp.concatenate([hi, lo], axis=1), w, preferred_element_type=F32)


def lanes(shape):
    return lax.broadcasted_iota(jnp.int32, shape, len(shape) - 1)


def edge_of(pack, p):
    return pltpu.roll(pack, (128 - H * p) % 128, 1) if p else pack


def taps(get, radius):
    total = weight(radius, 0) * get(0)
    for k in range(1, radius + 1):
        total = total + weight(radius, k) * (get(k) + get(-k))
    return total


def rows_band(radius, ny):
    y = lax.broadcasted_iota(jnp.int32, (ny, 2 * ny), 0)
    c = lax.broadcasted_iota(jnp.int32, (ny, 2 * ny), 1)
    d = jnp.where(c < ny, c, c - ny) - y
    value = (radius + 1) ** 2 - d * d
    return jnp.where(value > 0, value, 0).astype(F32).astype(BF16)


def ends_band():
    y = lax.broadcasted_iota(jnp.int32, (4 * H, 8 * H), 0)
    c = lax.broadcasted_iota(jnp.int32, (4 * H, 8 * H), 1)
    reach = jnp.where(y < 2 * H, R_SMALL + 1, R_LARGE + 1)
    same = (y < 2 * H) == (c < 4 * H)
    row, col = y % (2 * H), c % (2 * H)
    top = (row < H) == (col < H)
    d = jnp.where(row < H, col - H - row, col - row + H)
    value = reach * reach - d * d
    return jnp.where(same & top & (value > 0), value, 0).astype(F32).astype(BF16)


def level(small, large, e):
    low = e * (small * (0.25 * scale_of(R_SMALL))) + (0.5 - 0.25 * 0.3)
    high = e * (large * (0.25 * scale_of(R_LARGE))) + (0.5 - 0.25 * 0.1)
    return jnp.minimum(jnp.maximum(jnp.maximum(low, high), 0.0), 1.0)


def stack(m):
    hi = m.astype(BF16)
    lo = (m - hi.astype(F32)).astype(BF16)
    return jnp.concatenate([hi, lo], axis=0)


def x_halo(total, before, after, i, n, radius):
    for a in range(radius):
        d = i + radius - a
        if d <= radius:
            total = total + weight(radius, d) * before[a]
    for b in range(radius):
        d = n + b - i
        if d <= radius:
            total = total + weight(radius, d) * after[b]
    return total


def pack_body(d_hbm, d, zr, zl, xeu, xed, sems):
    snaps, nx, ny, nz = d.shape
    copies = [pltpu.make_async_copy(d_hbm.at[s], d.at[s], sems.at[s]) for s in range(snaps)]
    for copy in copies:
        copy.start()
    lane = lanes((ny, nz))
    for s in range(snaps):
        copies[s].wait()
        for out, at in ((xeu, nx - H), (xed, 0)):
            out[2 * s * H : (2 * s + 1) * H] = d[s, at : at + H, 0:H]
            out[(2 * s + 1) * H : (2 * s + 2) * H] = d[s, at : at + H, ny - H :]
        right = jnp.zeros((ny, nz), F32)
        left = jnp.zeros((ny, nz), F32)
        for x in range(nx):
            r = pltpu.roll(d[s, x], (H * x + H) % nz, 1)
            right = jnp.where((lane >= H * x) & (lane < H * x + H), r, right)
            at = (H * x + H) % nz
            left = jnp.where((lane >= at) & (lane < at + H), r, left)
        zr[s] = right
        zl[s] = pltpu.roll(left, nz - H, 1)


def second_body(za, zb, xzu, xzd):
    snaps, ny, nz = za.shape
    half = nz // 2
    lane = lanes((ny, nz))
    for s in range(snaps):
        xzu[s] = jnp.where(lane < half, pltpu.roll(za[s], half, 1), zb[s])
        xzd[s] = jnp.where(lane < half, za[s], pltpu.roll(zb[s], half, 1))


def inner_blocks(snaps, ny):
    return [(s, r * H) for s in range(snaps) for r in range(1, ny // H - 1)]


def slab_body(d, *outs):
    snaps, nx, ny, _ = d.shape
    jobs = inner_blocks(snaps, ny)
    for part, up, down in ((jobs[:-LATE], *outs[0:2]), (jobs[-LATE:], *outs[2:4])):
        for k, (s, row) in enumerate(part):
            up[k * H : (k + 1) * H] = d[s, nx - H :, row : row + H]
            down[k * H : (k + 1) * H] = d[s, 0:H, row : row + H]


def put(ref, s, i, r, value):
    ref[s, i, r : r + 8] = value


def x_sums(planes, store, radius):
    n = planes.shape[0] - 2 * H
    v = [planes[j] for j in range(n + 2 * H)]
    for i in range(n):
        store(i, taps(lambda k: v[H + i + k], radius))


def rim_body(d, xea, xeb, xza, xzd, xzu, xzb, ws, wl, yu, yd):
    snaps, nx, ny, nz = d.shape
    wm, we = band(False), band(True)

    def ends(v):
        return jnp.concatenate([v[0:H], v[ny - H :]], axis=0)

    for s in range(snaps):
        packs = [ends(p[s]) for p in (xza, xzd, xzu, xzb)]
        main = [xea[(s * 2 + h) * H + p] for p in range(H) for h in (0, 1)]
        main += [ends(d[s, x]) for x in range(nx)]
        main += [xeb[(s * 2 + h) * H + p] for p in range(H) for h in (0, 1)]
        side = [edge_of(packs[p // H], p % H) for p in range(nx + 2 * H)]
        out = mul(jnp.concatenate(main, axis=0), wm) + mul(jnp.concatenate(side, axis=0), we)
        out = out.reshape(nx + 2 * H, 2 * H, 2 * nz)
        for r in (0, H):
            x_sums(out[:, r : r + 8, :nz], lambda i, v: put(ws, s, i, r, v), R_SMALL)
            x_sums(out[:, r : r + 8, nz:], lambda i, v: put(wl, s, i, r, v), R_LARGE)
        small, large = ws[s], wl[s]
        yu[s, 0:nx] = large[:, H:]
        yd[s, 0:nx] = large[:, 0:H]
        half = nx // 2
        yu[s, nx:, 0:R_SMALL] = small[0:half, 2 * H - R_SMALL :]
        yu[s, nx:, R_SMALL:] = small[half:, 2 * H - R_SMALL :]
        yd[s, nx:, 0:R_SMALL] = small[0:half, 0:R_SMALL]
        yd[s, nx:, R_SMALL:] = small[half:, 0:R_SMALL]


def middle_body(d, xza, xzd, xzu, xzb, acc_s, acc_l, zs_all, zl_all):
    snaps, nx, ny, nz = d.shape
    wm, we = band(False), band(True)
    inner = ny - 2 * H

    for s in range(snaps):
        zs, zl = zs_all.at[s], zl_all.at[s]
        side = [edge_of(p[s, H : ny - H], k) for p in (xza, xzd, xzu, xzb) for k in range(H)]
        edge = mul(jnp.concatenate(side, axis=0), we).reshape(nx + 2 * H, inner, 2 * nz)
        main = mul(d[s, :, H : ny - H].reshape(nx * inner, nz), wm).reshape(nx, inner, 2 * nz)
        for ref, cut in ((zs, slice(0, nz)), (zl, slice(nz, 2 * nz))):
            ref[0:H] = edge[0:H, :, cut]
            ref[H : H + nx] = edge[H : H + nx, :, cut] + main[:, :, cut]
            ref[H + nx :] = edge[H + nx :, :, cut]
        for r in range(0, inner, 8):
            x_sums(zs[:, r : r + 8], lambda i, v: put(acc_s, s, i, r, v), R_SMALL)
            x_sums(zl[:, r : r + 8], lambda i, v: put(acc_l, s, i, r, v), R_LARGE)


def add_planes(xia, xib, acc_s, acc_l, us, ul, first, wm):
    nx, inner, nz = acc_s.shape
    cut = H - R_SMALL
    za = mul(xia.reshape(H * inner, nz), wm).reshape(inner // 8, H, 8, 2 * nz)
    zb = mul(xib.reshape(H * inner, nz), wm).reshape(inner // 8, H, 8, 2 * nz)
    for r in range(0, inner, 8):
        a, b = za[r // 8], zb[r // 8]
        at = slice(first + r, first + r + 8)
        for i in range(nx):
            us[i, at] = x_halo(
                acc_s[i, r : r + 8], a[cut:, :, :nz], b[:, :, :nz], i, nx, R_SMALL
            )
            ul[i, at] = x_halo(acc_l[i, r : r + 8], a[:, :, nz:], b[:, :, nz:], i, nx, R_LARGE)


def own_sums(us, ul, band_s, band_l, i):
    half = us.shape[0] // 2
    sums = []
    for ref, w in ((us, band_s), (ul, band_l)):
        pair = jnp.concatenate([stack(ref[i]), stack(ref[i + half])], axis=1)
        sums.append(jnp.dot(w, pair, preferred_element_type=F32))
    return sums


def halo_sums(ya, yb, s, i, half, w):
    top, bottom = ya[s, 2 * half + i], yb[s, 2 * half + i]
    first = jnp.concatenate([pltpu.roll(top, R_SMALL, 0), bottom], axis=0)
    second = jnp.concatenate([top, pltpu.roll(bottom, R_SMALL, 0)], axis=0)
    cols = []
    for at, small in ((i, first), (i + half, second)):
        large = jnp.concatenate([ya[s, at], yb[s, at]], axis=0)
        cols.append(jnp.concatenate([stack(small), stack(large)], axis=0))
    return jnp.dot(w, jnp.concatenate(cols, axis=1), preferred_element_type=F32)


def rim_rows(v):
    return jnp.concatenate([v[0:H], v[v.shape[0] - H :]], axis=0)


def prepare(xia, xib, acc_s, acc_l, ws, wl, us, ul, wm):
    ny = us.shape[1]
    add_planes(xia, xib, acc_s, acc_l, us, ul, H, wm)
    for ref, w in ((us, ws), (ul, wl)):
        ref[:, 0:H] = w[:, 0:H]
        ref[:, ny - H :] = w[:, H:]


def inner_body(xia, xib, acc_s, acc_l, ws, wl, eff, out, es, el, us, ul, done, sems):
    n, nx, ny, nz = us.shape
    half = nx // 2
    rows = slice(H, ny - H)
    wm = band(False)
    band_s, band_l = rows_band(R_SMALL, ny), rows_band(R_LARGE, ny)
    copies = []
    for j in range(n):
        s = j
        here = (acc_s.at[s], acc_l.at[s], ws.at[s], wl.at[s], us.at[j], ul.at[j])
        inner = ny - 2 * H
        got = [x[j * inner : (j + 1) * inner] for x in (xia, xib)]
        prepare(*got, *here, wm)
        for i in range(half):
            sums = own_sums(us.at[j], ul.at[j], band_s, band_l, i)
            for at, col in ((i, slice(0, nz)), (i + half, slice(nz, 2 * nz))):
                small, large = sums[0][:, col], sums[1][:, col]
                done[j, at] = level(small[rows], large[rows], eff[at, rows])
                es[j, at] = rim_rows(small)
                el[j, at] = rim_rows(large)
        copy = pltpu.make_async_copy(done.at[j], out.at[s, :, pl.ds(H, ny - 2 * H), :], sems.at[j])
        copy.start()
        copies.append(copy)
    for copy in copies:
        copy.wait()


def final_body(low, xia, xib, xja, xjb, acc_s, acc_l, ws, wl, eff, ya, yb, es, el, _, out, us, ul, rim, done, sems):
    n, nx, ny, nz = us.shape
    half = nx // 2
    wm, w = band(False), ends_band()
    band_s, band_l = rows_band(R_SMALL, ny), rows_band(R_LARGE, ny)
    sides = ((0, slice(0, nz)), (half, slice(nz, 2 * nz)))
    copies = []
    for s in range(low):
        for i in range(half):
            more = halo_sums(ya, yb, s, i, half, w)
            for step, col in sides:
                at = i + step
                add_s, add_l = more[0 : 2 * H, col], more[2 * H :, col]
                rim[s, at] = level(es[s, at] + add_s, el[s, at] + add_l, rim_rows(eff[at]))
        for k, start in enumerate((0, ny - H)):
            source = rim.at[s, :, pl.ds(k * H, H), :]
            target = out.at[s, :, pl.ds(start, H), :]
            copies.append(pltpu.make_async_copy(source, target, sems.at[len(copies)]))
            copies[-1].start()
    for j in range(n):
        s = low + j
        here = (acc_s.at[s], acc_l.at[s], ws.at[s], wl.at[s], us.at[j], ul.at[j])
        kept = low * (ny - 2 * H)
        got = [jnp.concatenate([x[kept:], y[...]], axis=0) for x, y in ((xia, xja), (xib, xjb))]
        prepare(*got, *here, wm)
        for i in range(half):
            sums = own_sums(us.at[j], ul.at[j], band_s, band_l, i)
            more = halo_sums(ya, yb, s, i, half, w)
            for step, col in sides:
                at = i + step
                small, large = sums[0][:, col], sums[1][:, col]
                add_s, add_l = more[0 : 2 * H, col], more[2 * H :, col]
                rows = slice(H, ny - H)
                done[j, at, rows] = level(small[rows], large[rows], eff[at, rows])
                ends = level(rim_rows(small) + add_s, rim_rows(large) + add_l, rim_rows(eff[at]))
                done[j, at, 0:H] = ends[0:H]
                done[j, at, ny - H :] = ends[H:]
            if i % 2:
                for step, _ in sides:
                    some = pl.ds(i - 1 + step, 2)
                    copies.append(
                        pltpu.make_async_copy(
                            done.at[j, some], out.at[s, some], sems.at[len(copies)]
                        )
                    )
                    copies[-1].start()
    for copy in copies:
        copy.wait()


def inner_call(high, args, shape):
    _, nx, ny, nz = shape
    ends = (high, nx, 2 * H, nz)
    return pl.pallas_call(
        inner_body,
        out_shape=[jax.ShapeDtypeStruct(shape, F32), pltpu.VMEM(ends, F32), pltpu.VMEM(ends, F32)],
        in_specs=[VMEM] * len(args),
        out_specs=[pl.BlockSpec(memory_space=pl.ANY), VMEM, VMEM],
        scratch_shapes=[pltpu.VMEM((high, nx, ny, nz), F32)] * 2
        + [pltpu.VMEM((high, nx, ny - 2 * H, nz), F32), pltpu.SemaphoreType.DMA((high,))],
        compiler_params=PARAMS,
        name="inner",
    )(*[near(a) for a in args])


def final_call(low, args, before, shape):
    snaps, nx, ny, nz = shape
    n = snaps - low
    any_space = pl.BlockSpec(memory_space=pl.ANY)
    return pl.pallas_call(
        lambda *refs: final_body(low, *refs),
        out_shape=jax.ShapeDtypeStruct(shape, F32),
        in_specs=[VMEM] * len(args) + [any_space],
        out_specs=any_space,
        scratch_shapes=[pltpu.VMEM((n, nx, ny, nz), F32)] * 2
        + [pltpu.VMEM((low, nx, 2 * H, nz), F32), pltpu.VMEM((n, nx, ny, nz), F32)]
        + [pltpu.SemaphoreType.DMA((n * nx // 2 + 2 * low,))],
        input_output_aliases={len(args): 0},
        compiler_params=PARAMS,
        name="final",
    )(*[near(a) for a in args], before)


def shift(block, axis, step):
    n = lax.axis_size(axis)
    return lax.ppermute(block, axis, [(i, (i + step) % n) for i in range(n)])


def both(axis, up, down):
    return shift(up, axis, 1), shift(down, axis, -1)


def steps(density, efficiency):
    block = density.shape
    snaps, nx, ny, nz = block
    inner = ny - 2 * H
    zpack = (snaps, ny, nz)
    xe = (2 * snaps * H, H, nz)
    own, zr, zl, xeu, xed = pl.pallas_call(
        pack_body,
        out_shape=[pltpu.VMEM(s, F32) for s in (block, zpack, zpack, xe, xe)],
        in_specs=[pl.BlockSpec(memory_space=pl.ANY)],
        out_specs=[VMEM] * 5,
        scratch_shapes=[pltpu.SemaphoreType.DMA((snaps,))],
        compiler_params=PARAMS,
        name="pack",
    )(pltpu.with_memory_space_constraint(density, pltpu.HBM))
    za, zb = both("gz", zr, zl)
    xea, xeb = both("gx", xeu, xed)
    blocks = (snaps * inner - LATE * H, LATE * H)
    slabs = [(n, H, nz) for n in blocks for _ in (0, 1)]
    slabs = run(slab_body, (own,), slabs)
    xzu, xzd = run(second_body, (za, zb), (zpack, zpack))
    xza, xzb = both("gx", xzu, xzd)
    halos = [both("gx", *slabs[2 * c : 2 * c + 2]) for c in (0, 1)]
    wide = nx + 2 * H
    rim = [(snaps, nx, 2 * H, nz)] * 2 + [(snaps, nx + nx // 2, H, nz)] * 2
    ws, wl, yu, yd = run(rim_body, (own, xea, xeb, xza, xzd, xzu, xzb), rim)
    ya, yb = both("gy", yu, yd)
    acc_s, acc_l = run(
        middle_body,
        (own, xza, xzd, xzu, xzb),
        [(snaps, nx, inner, nz)] * 2,
        [pltpu.VMEM((snaps, wide, inner, nz), F32)] * 2,
    )
    shared = (acc_s, acc_l, ws, wl, efficiency)
    out, es, el = inner_call(snaps - 1, halos[0] + shared, block)
    out = final_call(snaps - 1, halos[0] + halos[1] + shared + (ya, yb, es, el), out, block)
    return out


def solution(mesh):
    placed = (P(None, "gx", "gy", "gz"), P("gx", "gy", "gz"))
    return jax.shard_map(
        steps, mesh=mesh, in_specs=placed, out_specs=P(None, "gx", "gy", "gz"), check_vma=False
    )
```

```python
import math

import jax
import jax.numpy as jnp
from jax import lax
from jax.experimental import pallas as pl
from jax.experimental.pallas import tpu as pltpu
from jax.sharding import PartitionSpec as P


R_SMALL = 4
R_LARGE = 8
H = R_LARGE
LATE = 3
VMEM = pl.BlockSpec(memory_space=pltpu.VMEM)
F32 = jnp.float32
BF16 = jnp.bfloat16
PARAMS = pltpu.CompilerParams(vmem_limit_bytes=24 * 2**20)


def weight(radius, k):
    return float((radius + 1) ** 2 - k * k)


def scale_of(radius):
    n = float((radius + 1) ** 2)
    total = sum((1.0 - k * k / n) ** 2 for k in range(-radius, radius + 1))
    return (1.0 / (n * math.sqrt(total))) ** 3


def near(x):
    return pltpu.with_memory_space_constraint(x, pltpu.VMEM)


def run(body, args, outs, scratch=()):
    return pl.pallas_call(
        body,
        out_shape=[pltpu.VMEM(s, F32) for s in outs],
        in_specs=[VMEM] * len(args),
        out_specs=[VMEM] * len(outs),
        scratch_shapes=list(scratch),
        compiler_params=PARAMS,
    )(*[near(a) for a in args])


def band(edge):
    shape = (256, 256)
    row = lax.broadcasted_iota(jnp.int32, shape, 0) % 128
    col = lax.broadcasted_iota(jnp.int32, shape, 1)
    z = col % 128
    if edge:
        at = jnp.where(row < 64, row - H, 128 + row - 64)
        used = row % 64 < H
        d = at - z
    else:
        d = row - z
    reach = jnp.where(col < 128, R_SMALL + 1, R_LARGE + 1)
    value = reach * reach - d * d
    keep = value > 0
    if edge:
        keep = keep & used
    return jnp.where(keep, value, 0).astype(F32).astype(BF16)


def mul(m, w):
    hi = m.astype(BF16)
    lo = (m - hi.astype(F32)).astype(BF16)
    return jnp.dot(jnp.concatenate([hi, lo], axis=1), w, preferred_element_type=F32)


def lanes(shape):
    return lax.broadcasted_iota(jnp.int32, shape, len(shape) - 1)


def edge_of(pack, p):
    return pltpu.roll(pack, (128 - H * p) % 128, 1) if p else pack


def taps(get, radius):
    total = weight(radius, 0) * get(0)
    for k in range(1, radius + 1):
        total = total + weight(radius, k) * (get(k) + get(-k))
    return total


def rows_band(radius, ny):
    y = lax.broadcasted_iota(jnp.int32, (ny, 2 * ny), 0)
    c = lax.broadcasted_iota(jnp.int32, (ny, 2 * ny), 1)
    d = jnp.where(c < ny, c, c - ny) - y
    value = (radius + 1) ** 2 - d * d
    return jnp.where(value > 0, value, 0).astype(F32).astype(BF16)


def ends_band():
    y = lax.broadcasted_iota(jnp.int32, (4 * H, 8 * H), 0)
    c = lax.broadcasted_iota(jnp.int32, (4 * H, 8 * H), 1)
    reach = jnp.where(y < 2 * H, R_SMALL + 1, R_LARGE + 1)
    same = (y < 2 * H) == (c < 4 * H)
    row, col = y % (2 * H), c % (2 * H)
    top = (row < H) == (col < H)
    d = jnp.where(row < H, col - H - row, col - row + H)
    value = reach * reach - d * d
    return jnp.where(same & top & (value > 0), value, 0).astype(F32).astype(BF16)


def level(small, large, e):
    low = e * (small * (0.25 * scale_of(R_SMALL))) + (0.5 - 0.25 * 0.3)
    high = e * (large * (0.25 * scale_of(R_LARGE))) + (0.5 - 0.25 * 0.1)
    return jnp.minimum(jnp.maximum(jnp.maximum(low, high), 0.0), 1.0)


def stack(m):
    hi = m.astype(BF16)
    lo = (m - hi.astype(F32)).astype(BF16)
    return jnp.concatenate([hi, lo], axis=0)


def x_halo(total, before, after, i, n, radius):
    for a in range(radius):
        d = i + radius - a
        if d <= radius:
            total = total + weight(radius, d) * before[a]
    for b in range(radius):
        d = n + b - i
        if d <= radius:
            total = total + weight(radius, d) * after[b]
    return total


def pack_body(d_hbm, d, zr, zl, xeu, xed, sems):
    snaps, nx, ny, nz = d.shape
    copies = [pltpu.make_async_copy(d_hbm.at[s], d.at[s], sems.at[s]) for s in range(snaps)]
    for copy in copies:
        copy.start()
    lane = lanes((ny, nz))
    for s in range(snaps):
        copies[s].wait()
        for out, at in ((xeu, nx - H), (xed, 0)):
            out[2 * s * H : (2 * s + 1) * H] = d[s, at : at + H, 0:H]
            out[(2 * s + 1) * H : (2 * s + 2) * H] = d[s, at : at + H, ny - H :]
        right = jnp.zeros((ny, nz), F32)
        left = jnp.zeros((ny, nz), F32)
        for x in range(nx):
            r = pltpu.roll(d[s, x], (H * x + H) % nz, 1)
            right = jnp.where((lane >= H * x) & (lane < H * x + H), r, right)
            at = (H * x + H) % nz
            left = jnp.where((lane >= at) & (lane < at + H), r, left)
        zr[s] = right
        zl[s] = pltpu.roll(left, nz - H, 1)


def second_body(za, zb, xzu, xzd):
    snaps, ny, nz = za.shape
    half = nz // 2
    lane = lanes((ny, nz))
    for s in range(snaps):
        xzu[s] = jnp.where(lane < half, pltpu.roll(za[s], half, 1), zb[s])
        xzd[s] = jnp.where(lane < half, za[s], pltpu.roll(zb[s], half, 1))


def inner_blocks(snaps, ny):
    return [(s, r * H) for s in range(snaps) for r in range(1, ny // H - 1)]


def slab_body(d, *outs):
    snaps, nx, ny, _ = d.shape
    jobs = inner_blocks(snaps, ny)
    for part, up, down in ((jobs[:-LATE], *outs[0:2]), (jobs[-LATE:], *outs[2:4])):
        for k, (s, row) in enumerate(part):
            up[k * H : (k + 1) * H] = d[s, nx - H :, row : row + H]
            down[k * H : (k + 1) * H] = d[s, 0:H, row : row + H]


def put(ref, s, i, r, value):
    ref[s, i, r : r + 8] = value


def x_sums(planes, store, radius):
    n = planes.shape[0] - 2 * H
    v = [planes[j] for j in range(n + 2 * H)]
    for i in range(n):
        store(i, taps(lambda k: v[H + i + k], radius))


def rim_body(d, xea, xeb, xza, xzd, xzu, xzb, ws, wl, yu, yd):
    snaps, nx, ny, nz = d.shape
    wm, we = band(False), band(True)

    def ends(v):
        return jnp.concatenate([v[0:H], v[ny - H :]], axis=0)

    for s in range(snaps):
        packs = [ends(p[s]) for p in (xza, xzd, xzu, xzb)]
        main = [xea[(s * 2 + h) * H + p] for p in range(H) for h in (0, 1)]
        main += [ends(d[s, x]) for x in range(nx)]
        main += [xeb[(s * 2 + h) * H + p] for p in range(H) for h in (0, 1)]
        side = [edge_of(packs[p // H], p % H) for p in range(nx + 2 * H)]
        out = mul(jnp.concatenate(main, axis=0), wm) + mul(jnp.concatenate(side, axis=0), we)
        out = out.reshape(nx + 2 * H, 2 * H, 2 * nz)
        for r in (0, H):
            x_sums(out[:, r : r + 8, :nz], lambda i, v: put(ws, s, i, r, v), R_SMALL)
            x_sums(out[:, r : r + 8, nz:], lambda i, v: put(wl, s, i, r, v), R_LARGE)
        small, large = ws[s], wl[s]
        yu[s, 0:nx] = large[:, H:]
        yd[s, 0:nx] = large[:, 0:H]
        half = nx // 2
        yu[s, nx:, 0:R_SMALL] = small[0:half, 2 * H - R_SMALL :]
        yu[s, nx:, R_SMALL:] = small[half:, 2 * H - R_SMALL :]
        yd[s, nx:, 0:R_SMALL] = small[0:half, 0:R_SMALL]
        yd[s, nx:, R_SMALL:] = small[half:, 0:R_SMALL]


def middle_body(d, xza, xzd, xzu, xzb, acc_s, acc_l, zs_all, zl_all):
    snaps, nx, ny, nz = d.shape
    wm, we = band(False), band(True)
    inner = ny - 2 * H

    for s in range(snaps):
        zs, zl = zs_all.at[s], zl_all.at[s]
        side = [edge_of(p[s, H : ny - H], k) for p in (xza, xzd, xzu, xzb) for k in range(H)]
        edge = mul(jnp.concatenate(side, axis=0), we).reshape(nx + 2 * H, inner, 2 * nz)
        main = mul(d[s, :, H : ny - H].reshape(nx * inner, nz), wm).reshape(nx, inner, 2 * nz)
        for ref, cut in ((zs, slice(0, nz)), (zl, slice(nz, 2 * nz))):
            ref[0:H] = edge[0:H, :, cut]
            ref[H : H + nx] = edge[H : H + nx, :, cut] + main[:, :, cut]
            ref[H + nx :] = edge[H + nx :, :, cut]
        for r in range(0, inner, 8):
            x_sums(zs[:, r : r + 8], lambda i, v: put(acc_s, s, i, r, v), R_SMALL)
            x_sums(zl[:, r : r + 8], lambda i, v: put(acc_l, s, i, r, v), R_LARGE)


def add_planes(xia, xib, acc_s, acc_l, us, ul, first, wm):
    nx, inner, nz = acc_s.shape
    cut = H - R_SMALL
    za = mul(xia.reshape(H * inner, nz), wm).reshape(inner // 8, H, 8, 2 * nz)
    zb = mul(xib.reshape(H * inner, nz), wm).reshape(inner // 8, H, 8, 2 * nz)
    for r in range(0, inner, 8):
        a, b = za[r // 8], zb[r // 8]
        at = slice(first + r, first + r + 8)
        for i in range(nx):
            us[i, at] = x_halo(
                acc_s[i, r : r + 8], a[cut:, :, :nz], b[:, :, :nz], i, nx, R_SMALL
            )
            ul[i, at] = x_halo(acc_l[i, r : r + 8], a[:, :, nz:], b[:, :, nz:], i, nx, R_LARGE)


def own_sums(us, ul, band_s, band_l, i):
    half = us.shape[0] // 2
    sums = []
    for ref, w in ((us, band_s), (ul, band_l)):
        pair = jnp.concatenate([stack(ref[i]), stack(ref[i + half])], axis=1)
        sums.append(jnp.dot(w, pair, preferred_element_type=F32))
    return sums


def halo_sums(ya, yb, s, i, half, w):
    top, bottom = ya[s, 2 * half + i], yb[s, 2 * half + i]
    first = jnp.concatenate([pltpu.roll(top, R_SMALL, 0), bottom], axis=0)
    second = jnp.concatenate([top, pltpu.roll(bottom, R_SMALL, 0)], axis=0)
    cols = []
    for at, small in ((i, first), (i + half, second)):
        large = jnp.concatenate([ya[s, at], yb[s, at]], axis=0)
        cols.append(jnp.concatenate([stack(small), stack(large)], axis=0))
    return jnp.dot(w, jnp.concatenate(cols, axis=1), preferred_element_type=F32)


def rim_rows(v):
    return jnp.concatenate([v[0:H], v[v.shape[0] - H :]], axis=0)


def prepare(xia, xib, acc_s, acc_l, ws, wl, us, ul, wm):
    ny = us.shape[1]
    add_planes(xia, xib, acc_s, acc_l, us, ul, H, wm)
    for ref, w in ((us, ws), (ul, wl)):
        ref[:, 0:H] = w[:, 0:H]
        ref[:, ny - H :] = w[:, H:]


def inner_body(xia, xib, acc_s, acc_l, ws, wl, eff, done, es, el, us, ul):
    n, nx, ny, nz = us.shape
    half = nx // 2
    rows = slice(H, ny - H)
    wm = band(False)
    band_s, band_l = rows_band(R_SMALL, ny), rows_band(R_LARGE, ny)
    for j in range(n):
        s = j
        here = (acc_s.at[s], acc_l.at[s], ws.at[s], wl.at[s], us.at[j], ul.at[j])
        inner = ny - 2 * H
        got = [x[j * inner : (j + 1) * inner] for x in (xia, xib)]
        prepare(*got, *here, wm)
        for i in range(half):
            sums = own_sums(us.at[j], ul.at[j], band_s, band_l, i)
            for at, col in ((i, slice(0, nz)), (i + half, slice(nz, 2 * nz))):
                small, large = sums[0][:, col], sums[1][:, col]
                done[j, at] = level(small[rows], large[rows], eff[at, rows])
                es[j, at] = rim_rows(small)
                el[j, at] = rim_rows(large)


def final_body(low, xia, xib, xja, xjb, acc_s, acc_l, ws, wl, eff, ya, yb, kept_rows, es, el, out, us, ul, rim, done, sems):
    n, nx, ny, nz = us.shape
    half = nx // 2
    wm, w = band(False), ends_band()
    band_s, band_l = rows_band(R_SMALL, ny), rows_band(R_LARGE, ny)
    sides = ((0, slice(0, nz)), (half, slice(nz, 2 * nz)))
    copies = []
    for s in range(low):
        target = out.at[s, :, pl.ds(H, ny - 2 * H), :]
        copies.append(pltpu.make_async_copy(kept_rows.at[s], target, sems.at[len(copies)]))
        copies[-1].start()
    for s in range(low):
        for i in range(half):
            more = halo_sums(ya, yb, s, i, half, w)
            for step, col in sides:
                at = i + step
                add_s, add_l = more[0 : 2 * H, col], more[2 * H :, col]
                rim[s, at] = level(es[s, at] + add_s, el[s, at] + add_l, rim_rows(eff[at]))
        for k, start in enumerate((0, ny - H)):
            source = rim.at[s, :, pl.ds(k * H, H), :]
            target = out.at[s, :, pl.ds(start, H), :]
            copies.append(pltpu.make_async_copy(source, target, sems.at[len(copies)]))
            copies[-1].start()
    for j in range(n):
        s = low + j
        here = (acc_s.at[s], acc_l.at[s], ws.at[s], wl.at[s], us.at[j], ul.at[j])
        kept = low * (ny - 2 * H)
        got = [jnp.concatenate([x[kept:], y[...]], axis=0) for x, y in ((xia, xja), (xib, xjb))]
        prepare(*got, *here, wm)
        for i in range(half):
            sums = own_sums(us.at[j], ul.at[j], band_s, band_l, i)
            more = halo_sums(ya, yb, s, i, half, w)
            for step, col in sides:
                at = i + step
                small, large = sums[0][:, col], sums[1][:, col]
                add_s, add_l = more[0 : 2 * H, col], more[2 * H :, col]
                rows = slice(H, ny - H)
                done[j, at, rows] = level(small[rows], large[rows], eff[at, rows])
                ends = level(rim_rows(small) + add_s, rim_rows(large) + add_l, rim_rows(eff[at]))
                done[j, at, 0:H] = ends[0:H]
                done[j, at, ny - H :] = ends[H:]
            if i % 2:
                for step, _ in sides:
                    some = pl.ds(i - 1 + step, 2)
                    copies.append(
                        pltpu.make_async_copy(
                            done.at[j, some], out.at[s, some], sems.at[len(copies)]
                        )
                    )
                    copies[-1].start()
    for copy in copies:
        copy.wait()


def inner_call(high, args, shape):
    _, nx, ny, nz = shape
    outs = [(high, nx, ny - 2 * H, nz)] + [(high, nx, 2 * H, nz)] * 2
    return run(inner_body, args, outs, [pltpu.VMEM((high, nx, ny, nz), F32)] * 2)


def final_call(low, args, shape):
    snaps, nx, ny, nz = shape
    n = snaps - low
    return pl.pallas_call(
        lambda *refs: final_body(low, *refs),
        out_shape=jax.ShapeDtypeStruct(shape, F32),
        in_specs=[VMEM] * len(args),
        out_specs=pl.BlockSpec(memory_space=pl.ANY),
        scratch_shapes=[pltpu.VMEM((n, nx, ny, nz), F32)] * 2
        + [pltpu.VMEM((low, nx, 2 * H, nz), F32), pltpu.VMEM((n, nx, ny, nz), F32)]
        + [pltpu.SemaphoreType.DMA((n * nx // 2 + 3 * low,))],
        compiler_params=PARAMS,
        name="final",
    )(*[near(a) for a in args])


def shift(block, axis, step):
    n = lax.axis_size(axis)
    return lax.ppermute(block, axis, [(i, (i + step) % n) for i in range(n)])


def both(axis, up, down):
    return shift(up, axis, 1), shift(down, axis, -1)


def steps(density, efficiency):
    block = density.shape
    snaps, nx, ny, nz = block
    inner = ny - 2 * H
    zpack = (snaps, ny, nz)
    xe = (2 * snaps * H, H, nz)
    own, zr, zl, xeu, xed = pl.pallas_call(
        pack_body,
        out_shape=[pltpu.VMEM(s, F32) for s in (block, zpack, zpack, xe, xe)],
        in_specs=[pl.BlockSpec(memory_space=pl.ANY)],
        out_specs=[VMEM] * 5,
        scratch_shapes=[pltpu.SemaphoreType.DMA((snaps,))],
        compiler_params=PARAMS,
        name="pack",
    )(pltpu.with_memory_space_constraint(density, pltpu.HBM))
    za, zb = both("gz", zr, zl)
    xea, xeb = both("gx", xeu, xed)
    blocks = (snaps * inner - LATE * H, LATE * H)
    slabs = [(n, H, nz) for n in blocks for _ in (0, 1)]
    slabs = run(slab_body, (own,), slabs)
    xzu, xzd = run(second_body, (za, zb), (zpack, zpack))
    xza, xzb = both("gx", xzu, xzd)
    halos = [both("gx", *slabs[2 * c : 2 * c + 2]) for c in (0, 1)]
    wide = nx + 2 * H
    rim = [(snaps, nx, 2 * H, nz)] * 2 + [(snaps, nx + nx // 2, H, nz)] * 2
    ws, wl, yu, yd = run(rim_body, (own, xea, xeb, xza, xzd, xzu, xzb), rim)
    ya, yb = both("gy", yu, yd)
    acc_s, acc_l = run(
        middle_body,
        (own, xza, xzd, xzu, xzb),
        [(snaps, nx, inner, nz)] * 2,
        [pltpu.VMEM((snaps, wide, inner, nz), F32)] * 2,
    )
    shared = (acc_s, acc_l, ws, wl, efficiency)
    ready = inner_call(snaps - 1, halos[0] + shared, block)
    out = final_call(snaps - 1, halos[0] + halos[1] + shared + (ya, yb, *ready), block)
    return out


def solution(mesh):
    placed = (P(None, "gx", "gy", "gz"), P("gx", "gy", "gz"))
    return jax.shard_map(
        steps, mesh=mesh, in_specs=placed, out_specs=P(None, "gx", "gy", "gz"), check_vma=False
    )
```

```python
import math

import jax
import jax.numpy as jnp
from jax import lax
from jax.experimental import pallas as pl
from jax.experimental.pallas import tpu as pltpu
from jax.sharding import PartitionSpec as P


R_SMALL = 4
R_LARGE = 8
H = R_LARGE
LATE = 3
VMEM = pl.BlockSpec(memory_space=pltpu.VMEM)
F32 = jnp.float32
BF16 = jnp.bfloat16
PARAMS = pltpu.CompilerParams(vmem_limit_bytes=24 * 2**20)


def weight(radius, k):
    return float((radius + 1) ** 2 - k * k)


def scale_of(radius):
    n = float((radius + 1) ** 2)
    total = sum((1.0 - k * k / n) ** 2 for k in range(-radius, radius + 1))
    return (1.0 / (n * math.sqrt(total))) ** 3


def near(x):
    return pltpu.with_memory_space_constraint(x, pltpu.VMEM)


def run(body, args, outs, scratch=()):
    return pl.pallas_call(
        body,
        out_shape=[pltpu.VMEM(s, F32) for s in outs],
        in_specs=[VMEM] * len(args),
        out_specs=[VMEM] * len(outs),
        scratch_shapes=list(scratch),
        compiler_params=PARAMS,
    )(*[near(a) for a in args])


def band(edge):
    shape = (256, 256)
    row = lax.broadcasted_iota(jnp.int32, shape, 0) % 128
    col = lax.broadcasted_iota(jnp.int32, shape, 1)
    z = col % 128
    if edge:
        at = jnp.where(row < 64, row - H, 128 + row - 64)
        used = row % 64 < H
        d = at - z
    else:
        d = row - z
    reach = jnp.where(col < 128, R_SMALL + 1, R_LARGE + 1)
    value = reach * reach - d * d
    keep = value > 0
    if edge:
        keep = keep & used
    return jnp.where(keep, value, 0).astype(F32).astype(BF16)


def mul(m, w):
    hi = m.astype(BF16)
    lo = (m - hi.astype(F32)).astype(BF16)
    return jnp.dot(jnp.concatenate([hi, lo], axis=1), w, preferred_element_type=F32)


def lanes(shape):
    return lax.broadcasted_iota(jnp.int32, shape, len(shape) - 1)


def edge_of(pack, p):
    return pltpu.roll(pack, (128 - H * p) % 128, 1) if p else pack


def taps(get, radius):
    total = weight(radius, 0) * get(0)
    for k in range(1, radius + 1):
        total = total + weight(radius, k) * (get(k) + get(-k))
    return total


def rows_band(radius, ny):
    y = lax.broadcasted_iota(jnp.int32, (ny, 2 * ny), 0)
    c = lax.broadcasted_iota(jnp.int32, (ny, 2 * ny), 1)
    d = jnp.where(c < ny, c, c - ny) - y
    value = (radius + 1) ** 2 - d * d
    return jnp.where(value > 0, value, 0).astype(F32).astype(BF16)


def ends_band():
    y = lax.broadcasted_iota(jnp.int32, (4 * H, 8 * H), 0)
    c = lax.broadcasted_iota(jnp.int32, (4 * H, 8 * H), 1)
    reach = jnp.where(y < 2 * H, R_SMALL + 1, R_LARGE + 1)
    same = (y < 2 * H) == (c < 4 * H)
    row, col = y % (2 * H), c % (2 * H)
    top = (row < H) == (col < H)
    d = jnp.where(row < H, col - H - row, col - row + H)
    value = reach * reach - d * d
    return jnp.where(same & top & (value > 0), value, 0).astype(F32).astype(BF16)


def level(small, large, e):
    low = e * (small * (0.25 * scale_of(R_SMALL))) + (0.5 - 0.25 * 0.3)
    high = e * (large * (0.25 * scale_of(R_LARGE))) + (0.5 - 0.25 * 0.1)
    return jnp.minimum(jnp.maximum(jnp.maximum(low, high), 0.0), 1.0)


def stack(m):
    hi = m.astype(BF16)
    lo = (m - hi.astype(F32)).astype(BF16)
    return jnp.concatenate([hi, lo], axis=0)


def x_halo(total, before, after, i, n, radius):
    for a in range(radius):
        d = i + radius - a
        if d <= radius:
            total = total + weight(radius, d) * before[a]
    for b in range(radius):
        d = n + b - i
        if d <= radius:
            total = total + weight(radius, d) * after[b]
    return total


def pack_body(d_hbm, d, zr, zl, xeu, xed, sems):
    snaps, nx, ny, nz = d.shape
    copies = [pltpu.make_async_copy(d_hbm.at[s], d.at[s], sems.at[s]) for s in range(snaps)]
    for copy in copies:
        copy.start()
    lane = lanes((ny, nz))
    for s in range(snaps):
        copies[s].wait()
        for out, at in ((xeu, nx - H), (xed, 0)):
            out[2 * s * H : (2 * s + 1) * H] = d[s, at : at + H, 0:H]
            out[(2 * s + 1) * H : (2 * s + 2) * H] = d[s, at : at + H, ny - H :]
        right = jnp.zeros((ny, nz), F32)
        left = jnp.zeros((ny, nz), F32)
        for x in range(nx):
            r = pltpu.roll(d[s, x], (H * x + H) % nz, 1)
            right = jnp.where((lane >= H * x) & (lane < H * x + H), r, right)
            at = (H * x + H) % nz
            left = jnp.where((lane >= at) & (lane < at + H), r, left)
        zr[s] = right
        zl[s] = pltpu.roll(left, nz - H, 1)


def second_body(za, zb, xzu, xzd):
    snaps, ny, nz = za.shape
    half = nz // 2
    lane = lanes((ny, nz))
    for s in range(snaps):
        xzu[s] = jnp.where(lane < half, pltpu.roll(za[s], half, 1), zb[s])
        xzd[s] = jnp.where(lane < half, za[s], pltpu.roll(zb[s], half, 1))


def inner_blocks(snaps, ny):
    return [(s, r * H) for s in range(snaps) for r in range(1, ny // H - 1)]


def slab_body(d, *outs):
    snaps, nx, ny, _ = d.shape
    jobs = inner_blocks(snaps, ny)
    for part, up, down in ((jobs[:-LATE], *outs[0:2]), (jobs[-LATE:], *outs[2:4])):
        for k, (s, row) in enumerate(part):
            up[k * H : (k + 1) * H] = d[s, nx - H :, row : row + H]
            down[k * H : (k + 1) * H] = d[s, 0:H, row : row + H]


def put(ref, s, i, r, value):
    ref[s, i, r : r + 8] = value


def x_sums(planes, store, radius):
    n = planes.shape[0] - 2 * H
    v = [planes[j] for j in range(n + 2 * H)]
    for i in range(n):
        store(i, taps(lambda k: v[H + i + k], radius))


def rim_body(d, xea, xeb, xza, xzd, xzu, xzb, ws, wl, yu, yd):
    snaps, nx, ny, nz = d.shape
    wm, we = band(False), band(True)

    def ends(v):
        return jnp.concatenate([v[0:H], v[ny - H :]], axis=0)

    for s in range(snaps):
        packs = [ends(p[s]) for p in (xza, xzd, xzu, xzb)]
        main = [xea[(s * 2 + h) * H + p] for p in range(H) for h in (0, 1)]
        main += [ends(d[s, x]) for x in range(nx)]
        main += [xeb[(s * 2 + h) * H + p] for p in range(H) for h in (0, 1)]
        side = [edge_of(packs[p // H], p % H) for p in range(nx + 2 * H)]
        out = mul(jnp.concatenate(main, axis=0), wm) + mul(jnp.concatenate(side, axis=0), we)
        out = out.reshape(nx + 2 * H, 2 * H, 2 * nz)
        for r in (0, H):
            x_sums(out[:, r : r + 8, :nz], lambda i, v: put(ws, s, i, r, v), R_SMALL)
            x_sums(out[:, r : r + 8, nz:], lambda i, v: put(wl, s, i, r, v), R_LARGE)
        small, large = ws[s], wl[s]
        yu[s, 0:nx] = large[:, H:]
        yd[s, 0:nx] = large[:, 0:H]
        half = nx // 2
        yu[s, nx:, 0:R_SMALL] = small[0:half, 2 * H - R_SMALL :]
        yu[s, nx:, R_SMALL:] = small[half:, 2 * H - R_SMALL :]
        yd[s, nx:, 0:R_SMALL] = small[0:half, 0:R_SMALL]
        yd[s, nx:, R_SMALL:] = small[half:, 0:R_SMALL]


def middle_body(d, xza, xzd, xzu, xzb, acc_s, acc_l, zs_all, zl_all):
    snaps, nx, ny, nz = d.shape
    wm, we = band(False), band(True)
    inner = ny - 2 * H

    for s in range(snaps):
        zs, zl = zs_all.at[s], zl_all.at[s]
        side = [edge_of(p[s, H : ny - H], k) for p in (xza, xzd, xzu, xzb) for k in range(H)]
        edge = mul(jnp.concatenate(side, axis=0), we).reshape(nx + 2 * H, inner, 2 * nz)
        main = mul(d[s, :, H : ny - H].reshape(nx * inner, nz), wm).reshape(nx, inner, 2 * nz)
        for ref, cut in ((zs, slice(0, nz)), (zl, slice(nz, 2 * nz))):
            ref[0:H] = edge[0:H, :, cut]
            ref[H : H + nx] = edge[H : H + nx, :, cut] + main[:, :, cut]
            ref[H + nx :] = edge[H + nx :, :, cut]
        for r in range(0, inner, 8):
            x_sums(zs[:, r : r + 8], lambda i, v: put(acc_s, s, i, r, v), R_SMALL)
            x_sums(zl[:, r : r + 8], lambda i, v: put(acc_l, s, i, r, v), R_LARGE)


def add_planes(xia, xib, acc_s, acc_l, us, ul, first, wm):
    nx, inner, nz = acc_s.shape
    cut = H - R_SMALL
    za = mul(xia.reshape(H * inner, nz), wm).reshape(inner // 8, H, 8, 2 * nz)
    zb = mul(xib.reshape(H * inner, nz), wm).reshape(inner // 8, H, 8, 2 * nz)
    for r in range(0, inner, 8):
        a, b = za[r // 8], zb[r // 8]
        at = slice(first + r, first + r + 8)
        for i in range(nx):
            us[i, at] = x_halo(
                acc_s[i, r : r + 8], a[cut:, :, :nz], b[:, :, :nz], i, nx, R_SMALL
            )
            ul[i, at] = x_halo(acc_l[i, r : r + 8], a[:, :, nz:], b[:, :, nz:], i, nx, R_LARGE)


def own_sums(us, ul, band_s, band_l, i):
    half = us.shape[0] // 2
    sums = []
    for ref, w in ((us, band_s), (ul, band_l)):
        pair = jnp.concatenate([stack(ref[i]), stack(ref[i + half])], axis=1)
        sums.append(jnp.dot(w, pair, preferred_element_type=F32))
    return sums


def halo_sums(ya, yb, s, i, half, w):
    top, bottom = ya[s, 2 * half + i], yb[s, 2 * half + i]
    first = jnp.concatenate([pltpu.roll(top, R_SMALL, 0), bottom], axis=0)
    second = jnp.concatenate([top, pltpu.roll(bottom, R_SMALL, 0)], axis=0)
    cols = []
    for at, small in ((i, first), (i + half, second)):
        large = jnp.concatenate([ya[s, at], yb[s, at]], axis=0)
        cols.append(jnp.concatenate([stack(small), stack(large)], axis=0))
    return jnp.dot(w, jnp.concatenate(cols, axis=1), preferred_element_type=F32)


def rim_rows(v):
    return jnp.concatenate([v[0:H], v[v.shape[0] - H :]], axis=0)


def prepare(xia, xib, acc_s, acc_l, ws, wl, us, ul, wm):
    ny = us.shape[1]
    add_planes(xia, xib, acc_s, acc_l, us, ul, H, wm)
    for ref, w in ((us, ws), (ul, wl)):
        ref[:, 0:H] = w[:, 0:H]
        ref[:, ny - H :] = w[:, H:]


def inner_body(low, xia, xib, *refs):
    late, refs = (refs[:2], refs[2:]) if low else ((), refs)
    acc_s, acc_l, ws, wl, eff = refs[:5]
    done, es, el, us, ul = refs[-5:]
    n, nx, ny, nz = us.shape
    half = nx // 2
    inner = ny - 2 * H
    rows = slice(H, ny - H)
    wm = band(False)
    band_s, band_l = rows_band(R_SMALL, ny), rows_band(R_LARGE, ny)
    for j in range(n):
        s = low + j
        here = (acc_s.at[s], acc_l.at[s], ws.at[s], wl.at[s], us.at[j], ul.at[j])
        got = [x[s * inner : min((s + 1) * inner, x.shape[0])] for x in (xia, xib)]
        if late:
            got = [jnp.concatenate([x, y[...]], axis=0) for x, y in zip(got, late)]
        prepare(*got, *here, wm)
        for i in range(half):
            sums = own_sums(us.at[j], ul.at[j], band_s, band_l, i)
            for at, col in ((i, slice(0, nz)), (i + half, slice(nz, 2 * nz))):
                small, large = sums[0][:, col], sums[1][:, col]
                done[j, at] = level(small[rows], large[rows], eff[at, rows])
                es[j, at] = rim_rows(small)
                el[j, at] = rim_rows(large)


def ends_body(eff, ya, yb, *refs):
    out, rim, sems = refs[-3:]
    parts = refs[:-3]
    ny, nz = eff.shape[1:]
    half = eff.shape[0] // 2
    w = ends_band()
    trios = list(zip(parts[0::3], parts[1::3], parts[2::3]))
    sums = [(es.at[j], el.at[j]) for _, es, el in trios for j in range(es.shape[0])]
    copies = []
    first = 0
    for ready, _, _ in trios:
        n = ready.shape[0]
        target = out.at[pl.ds(first, n), :, pl.ds(H, ny - 2 * H), :]
        copies.append(pltpu.make_async_copy(ready, target, sems.at[len(copies)]))
        copies[-1].start()
        first += n
    for s, (es, el) in enumerate(sums):
        for i in range(half):
            more = halo_sums(ya, yb, s, i, half, w)
            for at, col in ((i, slice(0, nz)), (i + half, slice(nz, 2 * nz))):
                add_s, add_l = more[0 : 2 * H, col], more[2 * H :, col]
                rim[s, at] = level(es[at] + add_s, el[at] + add_l, rim_rows(eff[at]))
        for k, start in enumerate((0, ny - H)):
            source = rim.at[s, :, pl.ds(k * H, H), :]
            target = out.at[s, :, pl.ds(start, H), :]
            copies.append(pltpu.make_async_copy(source, target, sems.at[len(copies)]))
            copies[-1].start()
    for copy in copies:
        copy.wait()


def inner_call(low, high, args, shape):
    _, nx, ny, nz = shape
    n = high - low
    outs = [(n, nx, ny - 2 * H, nz)] + [(n, nx, 2 * H, nz)] * 2
    scratch = [pltpu.VMEM((n, nx, ny, nz), F32)] * 2
    return run(lambda *refs: inner_body(low, *refs), args, outs, scratch)


def ends_call(args, shape):
    snaps, nx, _, nz = shape
    return pl.pallas_call(
        ends_body,
        out_shape=jax.ShapeDtypeStruct(shape, F32),
        in_specs=[VMEM] * len(args),
        out_specs=pl.BlockSpec(memory_space=pl.ANY),
        scratch_shapes=[
            pltpu.VMEM((snaps, nx, 2 * H, nz), F32),
            pltpu.SemaphoreType.DMA((2 * snaps + 2,)),
        ],
        compiler_params=PARAMS,
        name="ends",
    )(*[near(a) for a in args])


def shift(block, axis, step):
    n = lax.axis_size(axis)
    return lax.ppermute(block, axis, [(i, (i + step) % n) for i in range(n)])


def both(axis, up, down):
    return shift(up, axis, 1), shift(down, axis, -1)


def steps(density, efficiency):
    block = density.shape
    snaps, nx, ny, nz = block
    inner = ny - 2 * H
    zpack = (snaps, ny, nz)
    xe = (2 * snaps * H, H, nz)
    own, zr, zl, xeu, xed = pl.pallas_call(
        pack_body,
        out_shape=[pltpu.VMEM(s, F32) for s in (block, zpack, zpack, xe, xe)],
        in_specs=[pl.BlockSpec(memory_space=pl.ANY)],
        out_specs=[VMEM] * 5,
        scratch_shapes=[pltpu.SemaphoreType.DMA((snaps,))],
        compiler_params=PARAMS,
        name="pack",
    )(pltpu.with_memory_space_constraint(density, pltpu.HBM))
    za, zb = both("gz", zr, zl)
    xea, xeb = both("gx", xeu, xed)
    blocks = (snaps * inner - LATE * H, LATE * H)
    slabs = [(n, H, nz) for n in blocks for _ in (0, 1)]
    slabs = run(slab_body, (own,), slabs)
    xzu, xzd = run(second_body, (za, zb), (zpack, zpack))
    xza, xzb = both("gx", xzu, xzd)
    halos = [both("gx", *slabs[2 * c : 2 * c + 2]) for c in (0, 1)]
    wide = nx + 2 * H
    rim = [(snaps, nx, 2 * H, nz)] * 2 + [(snaps, nx + nx // 2, H, nz)] * 2
    ws, wl, yu, yd = run(rim_body, (own, xea, xeb, xza, xzd, xzu, xzb), rim)
    ya, yb = both("gy", yu, yd)
    acc_s, acc_l = run(
        middle_body,
        (own, xza, xzd, xzu, xzb),
        [(snaps, nx, inner, nz)] * 2,
        [pltpu.VMEM((snaps, wide, inner, nz), F32)] * 2,
    )
    shared = (acc_s, acc_l, ws, wl, efficiency)
    last = snaps - 1
    first = inner_call(0, last, halos[0] + shared, block)
    second = inner_call(last, snaps, halos[0] + halos[1] + shared, block)
    out = ends_call((efficiency, ya, yb, *first, *second), block)
    return out


def solution(mesh):
    placed = (P(None, "gx", "gy", "gz"), P("gx", "gy", "gz"))
    return jax.shard_map(
        steps, mesh=mesh, in_specs=placed, out_specs=P(None, "gx", "gy", "gz"), check_vma=False
    )
```
